512 devices in a mesh: blk: 64 (over x, y, core), phe: 8 (over z).
Axes of the slice: x: 4, y: 8, z: 8, core: 2. Of those that a mesh axis runs over, the one named last changes fastest.
Arguments:
- ld_rows: bfloat16 [65536, 1024], P('blk'), may hold values from -1.5 to 1.5, as said below
- block_first: int32 [65536], P('blk'), may hold values from 0 to 65535, as said below
- beta_hat: float32 [512, 65536], P('phe', 'blk'), may hold values from -6 to 6
- psi: float32 [512, 65536], P('phe', 'blk'), may hold values from 0.05 to 5
- noise: bfloat16 [3, 512, 65536], P(None, 'phe', 'blk'), may hold values from -5 to 5
- sample_size: int32 [512], P('phe'), may hold values from 2000 to 199999
Outputs:
- effects: float32 [512, 65536], P('phe', 'blk')
The draws below stay inside these ranges and needn't reach their ends.
Inputs may be any that keep to these rules, and one draw needn't show every extreme that they name: block_first[j] is the first SNP of the run of consecutive SNPs that forms j's LD block; every block holds 128 to 1024 SNPs, except the last block, which ends at SNP 65536 - 1 and may hold fewer. ld_rows[j, c] is the LD between SNP j and SNP block_first[j] + c for c below the length of j's block, and zero for larger c; every block's matrix is symmetric with unit diagonal.
All inputs are finite; a program needn't handle non-finite values.
Results may differ from the reference program's by a relative error of at most 0.00055.
The reference program's roundings to bfloat16 on the way count: a program that leaves them out, or rounds other values in their place, can miss the bound.
Values may be sent and summed in bfloat16 or wider, within the bound.
A program may use at most 64 MiB of HBM per device.

```python
import math
import jax
import jax.numpy as jnp
from jax import lax

BMAX = 1024
MINB = 128
ITERS = 3
NSNP = 65536
PHENO = 512


def block_layout(key):
    count = NSNP // MINB + 2
    lengths = jax.random.randint(jax.random.fold_in(key, 11), (count,), MINB, BMAX + 1).astype(jnp.int32)
    endings = jnp.cumsum(lengths).astype(jnp.int32)
    beginnings = endings - lengths
    positions = jnp.arange(NSNP, dtype=jnp.int32)
    member = jnp.searchsorted(endings, positions, side='right')
    first_snp = beginnings[member]
    block_size = jnp.minimum(endings[member], NSNP) - first_snp
    return (first_snp, block_size)


def draw_block_first(key, part):
    return block_layout(key)[0].astype(jnp.int32)


def draw_ld_rows(key, part):
    first_snp, block_size = block_layout(key)
    positions = jnp.arange(NSNP, dtype=jnp.int32)
    base_draw = jnp.clip(jax.random.normal(jax.random.fold_in(key, 12), (NSNP, BMAX), jnp.float32), -4.0, 4.0)
    offsets = jnp.arange(BMAX, dtype=jnp.int32)
    columns = first_snp[:, None] + offsets[None, :]
    inside = offsets[None, :] < block_size[:, None]
    mirror = base_draw[jnp.clip(columns, 0, NSNP - 1), (positions - first_snp)[:, None]]
    spread = 0.35 / math.sqrt(2.0) / jnp.sqrt(block_size.astype(jnp.float32))
    values = (base_draw + mirror) * spread[:, None]
    values = jnp.where(columns == positions[:, None], 1.0, values)
    values = jnp.where(inside, values, 0.0)
    return values.astype(jnp.bfloat16)


def touch_ends(entries, rng, least, high):
    index_at = [jax.random.randint(jax.random.fold_in(rng, axis), (), 0, length) for axis, length in enumerate(entries.shape)]
    longest = entries.shape.index(max(entries.shape))
    neighbour = index_at[:longest] + [(index_at[longest] + 1) % entries.shape[longest]] + index_at[longest + 1:]
    return entries.at[tuple(index_at)].set(least).at[tuple(neighbour)].set(high)


def block_levels(stream_key, shape, shards, smallest, top_value):
    def one(axis_at, blocks):
        heights = jax.random.uniform(jax.random.fold_in(jax.random.fold_in(stream_key, 6), axis_at), (blocks,), jnp.float32, smallest / len(shards), top_value / len(shards))
        return jnp.repeat(jnp.exp(heights), shape[axis_at] // blocks).reshape((-1,) + (1,) * (len(shape) - axis_at - 1))

    factor_of = one(*shards[0])
    for cut in shards[1:]:
        factor_of = factor_of * one(*cut)
    return factor_of


def gaussian(own_key, shape, deviation, limit, shards=(), held_as=jnp.bfloat16):
    values = deviation * jax.random.normal(own_key, shape, jnp.float32)
    if shards:
        values = values * block_levels(own_key, shape, shards, -0.22, 0.18)
    return jnp.clip(values, -limit, limit).astype(held_as)


def setup_inputs(seed: int = 0) -> dict:
    key_of = jax.random.split(jax.random.key(seed), 7)
    ld_rows = draw_ld_rows(jax.random.fold_in(key_of[6], 71), 0)
    block_first = draw_block_first(jax.random.fold_in(key_of[6], 71), 0)
    beta_hat = gaussian(key_of[2], (PHENO, NSNP), 1.0, 6.0, ((0, 8), (1, 64)), jnp.float32)
    psi = jnp.clip(jnp.exp(math.log(5.0) - 4.6051702 * jax.random.uniform(key_of[3], (PHENO, NSNP), jnp.float32) ** block_levels(key_of[3], (PHENO, NSNP), ((0, 8), (1, 64)), -0.2, 0.2)), 0.05, 5.0)
    noise = gaussian(key_of[4], (ITERS, PHENO, NSNP), 1.0, 5.0, ((1, 8), (2, 64)))
    sample_size = touch_ends(jax.random.randint(key_of[5], (PHENO,), 2000, 200000), jax.random.fold_in(key_of[5], 1), 2000, 199999).astype(jnp.int32)
    return dict(ld_rows=ld_rows, block_first=block_first, beta_hat=beta_hat, psi=psi, noise=noise, sample_size=sample_size)


tiny_term = 1e-06
sample_ref = 20000.0

def apply_blocks(rounded, ld_rows, block_first):
    positions = jnp.arange(NSNP, dtype=jnp.int32)
    starting = jnp.nonzero(block_first == positions, size=NSNP // MINB + 2, fill_value=NSNP)[0].astype(jnp.int32)
    block_count = jnp.sum((block_first == positions).astype(jnp.int32))
    following = jnp.concatenate([starting[1:], jnp.full((1,), NSNP, jnp.int32)])
    lengths = following - starting
    ld_padded = jnp.pad(ld_rows, ((0, BMAX), (0, 0)))
    low_padded = jnp.pad(rounded, ((0, 0), (0, BMAX)))
    offsets = jnp.arange(BMAX, dtype=jnp.int32)

    def one_block(number, result):
        row_start = starting[number]
        ld_tile = lax.dynamic_slice_in_dim(ld_padded, row_start, BMAX, 0)
        window = lax.dynamic_slice_in_dim(low_padded, row_start, BMAX, 1)
        product = lax.dot_general(window, ld_tile, (((1,), (1,)), ((), ())), preferred_element_type=jnp.float32)
        product = jnp.where((offsets < lengths[number])[None, :], product, jnp.float32(0.0))
        current = lax.dynamic_slice_in_dim(result, row_start, BMAX, 1)
        return lax.dynamic_update_slice_in_dim(result, current + product, row_start, 1)
    start_value = jnp.zeros((rounded.shape[0], NSNP + BMAX), jnp.float32)
    result = lax.fori_loop(0, block_count, one_block, start_value)
    return result[:, :NSNP]

def reference(ld_rows, block_first, beta_hat, psi, noise, sample_size):
    beta = jnp.zeros(beta_hat.shape, jnp.float32)
    for iteration in range(ITERS):
        rounded = beta.astype(jnp.bfloat16)
        grad = beta_hat - apply_blocks(rounded, ld_rows, block_first)
        resid = lax.optimization_barrier(jnp.sum(grad * grad, axis=1)) / NSNP + tiny_term
        weighted = beta * beta / psi
        scale = lax.optimization_barrier(jnp.sum(weighted, axis=1)) / NSNP + tiny_term
        pooled = jnp.sum(weighted) / (NSNP * PHENO) + tiny_term
        phi = (scale + pooled) / 2.0
        amp = jnp.sqrt(resid * sample_ref / sample_size.astype(jnp.float32))
        shrink = psi / (psi + phi[:, None])
        beta = shrink * (beta + grad + amp[:, None] * noise[iteration].astype(jnp.float32))
    return beta
```

```python
import functools

import jax
import jax.numpy as jnp
from jax import lax
from jax.experimental import pallas as pl
from jax.experimental.pallas import tpu as pltpu
from jax.sharding import PartitionSpec as P

ITERS = 3
TINY = 1e-06
SAMPLE_REF = 20000.0
MESH = pl.DeviceIdType.MESH
LANES = 128
NB = 8
CH = 256
NCH = 4


def peer_offsets(nx, ny):
    def hops(d):
        dx, dy, dc = d
        return min(dx, nx - dx) + min(dy, ny - dy) + 0.2 * dc

    every = [(dx, dy, dc) for dx in range(nx) for dy in range(ny) for dc in range(2)]
    return sorted([d for d in every if d != (0, 0, 0)], key=lambda d: -hops(d))


def kernel(
    nx, ny, nz, snps,
    ld_hbm, bf_hbm, bh_hbm, psi_hbm, nz_hbm, ss_hbm,
    u_hbm, v_hbm, amp_hbm,
    ld_v, bf_s, bh_v, psi_v, nz_v, ss_v,
    own_m, halo_m, dl_m, dr_m,
    beta_v, low_v, left_v, right_v, acc_v, t_v, sh_v, u_v, v_v, amp_v,
    rbuf, sbuf, pbuf,
    in_sem, out_sem, rs_sem, rr_sem, ss_sem, sr_sem, ps_sem, pr_sem,
    ls_sem, lr_sem, qs_sem, qr_sem,
):
    nblk = nx * ny * 2
    me = lax.axis_index("blk")
    mz = lax.axis_index("phe")
    mx, my, mc = me // (2 * ny), (me // 2) % ny, me % 2
    offsets = peer_offsets(nx, ny)

    def blk_of(d):
        dx, dy, dc = d
        return ((mx + dx) % nx) * (2 * ny) + ((my + dy) % ny) * 2 + (mc + dc) % 2

    barrier = pltpu.get_barrier_semaphore()
    for d in offsets:
        pl.semaphore_signal(barrier, inc=1, device_id={"blk": blk_of(d)}, device_id_type=MESH)
    for dz in range(1, nz):
        pl.semaphore_signal(barrier, inc=1, device_id={"phe": (mz + dz) % nz}, device_id_type=MESH)

    loads = [
        pltpu.make_async_copy(bh_hbm, bh_v, in_sem.at[0]),
        pltpu.make_async_copy(bf_hbm, bf_s, in_sem.at[1]),
        pltpu.make_async_copy(ld_hbm, ld_v, in_sem.at[2]),
        pltpu.make_async_copy(psi_hbm, psi_v, in_sem.at[3]),
        pltpu.make_async_copy(nz_hbm, nz_v, in_sem.at[4]),
        pltpu.make_async_copy(ss_hbm, ss_v, in_sem.at[5]),
    ]
    for copy in loads:
        copy.start()

    def cols(k):
        return slice(k * LANES, (k + 1) * LANES)

    def as_row(first, second):
        both = jnp.concatenate([first, second], axis=0)
        return jnp.sum(both.T, axis=0, keepdims=True)

    def as_col(row):
        return jnp.broadcast_to(row, (LANES, LANES)).T[:64]

    def exchange_start(buf, t, ssem, rsem, row):
        buf[t, pl.ds(me, 1)] = row
        for d in offsets:
            pltpu.make_async_remote_copy(
                buf.at[t, pl.ds(me, 1)], buf.at[t, pl.ds(me, 1)], ssem.at[t], rsem.at[t],
                device_id={"blk": blk_of(d)}, device_id_type=MESH,
            ).start()

    def rows_wait(buf, t, n, sem):
        part = buf.at[t, pl.ds(0, n)]
        pltpu.make_async_copy(part, part, sem.at[t]).wait()

    def exchange_finish(buf, t, rsem):
        rows_wait(buf, t, nblk - 1, rsem)
        return jnp.sum(buf[t], axis=0, keepdims=True)

    loads[0].wait()
    zero = jnp.zeros((64, LANES), jnp.float32)
    acc = zero
    for k in range(NB):
        b = bh_v[:, cols(k)]
        acc = acc + b * b
    row0 = as_row(acc, zero)
    pl.semaphore_wait(barrier, nblk - 1 + nz - 1)
    exchange_start(rbuf, 0, rs_sem, rr_sem, row0)

    loads[1].wait()
    loads[2].wait()
    base = me * snps
    lane = lax.broadcasted_iota(jnp.int32, (LANES, snps), 1)
    sub = lax.broadcasted_iota(jnp.int32, (LANES, snps), 0)
    for i in range(NB):
        rows = slice(i * LANES, (i + 1) * LANES)
        first = bf_s[i * LANES]
        last = bf_s[i * LANES + LANES - 1]
        tile = ld_v[rows, :].astype(jnp.float32)
        ta = first & (snps - 1)
        tb = last & (snps - 1)
        ra = pltpu.roll(tile, ta, axis=1)
        rb = pltpu.roll(tile, tb, axis=1)
        split = jnp.where(last == first, LANES, last - base - i * LANES)
        in_b = sub >= split
        moved = jnp.where(in_b, rb, ra)
        thr = jnp.where(in_b, tb, ta)
        below = jnp.where(lane < thr, 1, 0)
        crossing = jnp.where(first < base, 1, 0)
        left_seg = jnp.where(in_b, 0, crossing)
        own = jnp.where(below == left_seg, moved, 0.0)
        own_m[rows, :] = own.astype(jnp.bfloat16)
        halo_m[:, rows] = (moved - own).T.astype(jnp.bfloat16)
    qi = lax.broadcasted_iota(jnp.int32, (CH, CH), 0)
    ji = lax.broadcasted_iota(jnp.int32, (CH, CH), 1)
    for k in range(NCH):
        part = slice(k * CH, (k + 1) * CH)
        h = halo_m[part, part].astype(jnp.float32)
        dl_m[k] = jnp.where(qi > ji, h, 0.0).astype(jnp.bfloat16)
        dr_m[k] = jnp.where(qi < ji, h, 0.0).astype(jnp.bfloat16)

    loads[3].wait()
    loads[4].wait()
    loads[5].wait()
    ss = ss_v[...].astype(jnp.float32)
    ss2 = jnp.concatenate([ss, ss], axis=1)
    for k in range(NB):
        psi = psi_v[:, cols(k)]
        sh_v[:, cols(k)] = psi / (psi + TINY)
        t_v[:, cols(k)] = bh_v[:, cols(k)]

    right_peer = (me + 1) % nblk
    left_peer = (me + nblk - 1) % nblk
    nsnp = float(snps * nblk)

    for t in range(1, ITERS):
        total = exchange_finish(rbuf, t - 1, rr_sem)
        resid = total / nsnp + TINY
        amp = as_col(jnp.sqrt(resid * SAMPLE_REF / ss2))
        h = t - 1
        sacc = zero
        for k in range(NB):
            b = sh_v[:, cols(k)] * (t_v[:, cols(k)] + amp * nz_v[t - 1, :, cols(k)].astype(jnp.float32))
            beta_v[:, cols(k)] = b
            low_v[h, k // 2, :, (k % 2) * LANES:(k % 2 + 1) * LANES] = b.astype(jnp.bfloat16)
            sacc = sacc + b * b / psi_v[:, cols(k)]

        halo = []
        for k in range(NCH):
            kr, kl = NCH - 1 - k, k
            to_right = pltpu.make_async_remote_copy(
                low_v.at[h, kr], left_v.at[h, kr], ls_sem.at[h, kr], lr_sem.at[h, kr],
                device_id={"blk": right_peer}, device_id_type=MESH,
            )
            to_left = pltpu.make_async_remote_copy(
                low_v.at[h, kl], right_v.at[h, kl], qs_sem.at[h, kl], qr_sem.at[h, kl],
                device_id={"blk": left_peer}, device_id_type=MESH,
            )
            to_right.start()
            to_left.start()
            halo.append((kr, kl, to_right, to_left))
        exchange_start(sbuf, h, ss_sem, sr_sem, as_row(sacc, zero))

        prod = jnp.dot(low_v[h, 0], own_m[0:CH, :], preferred_element_type=jnp.float32)
        for k in range(1, NCH):
            prod = prod + jnp.dot(low_v[h, k], own_m[k * CH:(k + 1) * CH, :], preferred_element_type=jnp.float32)
        acc_v[...] = prod
        for kr, kl, to_right, to_left in halo:
            to_right.wait_recv()
            x = left_v[h, kr]
            here = slice(kr * CH, (kr + 1) * CH)
            if kr:
                acc_v[:, :kr * CH] += jnp.dot(x, halo_m[here, :kr * CH], preferred_element_type=jnp.float32)
            acc_v[:, here] += jnp.dot(x, dl_m[kr], preferred_element_type=jnp.float32)
            to_left.wait_recv()
            x = right_v[h, kl]
            here = slice(kl * CH, (kl + 1) * CH)
            if kl < NCH - 1:
                acc_v[:, (kl + 1) * CH:] += jnp.dot(x, halo_m[here, (kl + 1) * CH:], preferred_element_type=jnp.float32)
            acc_v[:, here] += jnp.dot(x, dr_m[kl], preferred_element_type=jnp.float32)

        racc = zero
        for k in range(NB):
            g = bh_v[:, cols(k)] - acc_v[:, cols(k)]
            racc = racc + g * g
            t_v[:, cols(k)] = beta_v[:, cols(k)] + g
        exchange_start(rbuf, t, rs_sem, rr_sem, as_row(racc, zero))

        stotal = exchange_finish(sbuf, h, sr_sem)
        mine = jnp.sum(stotal, axis=1, keepdims=True)
        pbuf[h, pl.ds(mz, 1)] = jnp.broadcast_to(mine, (1, LANES))
        for dz in range(1, nz):
            pltpu.make_async_remote_copy(
                pbuf.at[h, pl.ds(mz, 1)], pbuf.at[h, pl.ds(mz, 1)], ps_sem.at[h], pr_sem.at[h],
                device_id={"phe": (mz + dz) % nz}, device_id_type=MESH,
            ).start()
        rows_wait(pbuf, h, nz - 1, pr_sem)
        pooled = jnp.sum(pbuf[h], axis=0, keepdims=True) / (nsnp * (64 * nz)) + TINY
        scale = stotal / nsnp + TINY
        phi = as_col((scale + pooled) / 2.0)
        for k in range(NB):
            psi = psi_v[:, cols(k)]
            shrink = psi / (psi + phi)
            sh_v[:, cols(k)] = shrink
            if t == ITERS - 1:
                u_v[:, cols(k)] = shrink * t_v[:, cols(k)]
                v_v[:, cols(k)] = shrink * nz_v[t, :, cols(k)].astype(jnp.float32)

    outs = [
        pltpu.make_async_copy(u_v, u_hbm, out_sem.at[0]),
        pltpu.make_async_copy(v_v, v_hbm, out_sem.at[1]),
    ]
    for copy in outs:
        copy.start()
    total = exchange_finish(rbuf, ITERS - 1, rr_sem)
    resid = total / nsnp + TINY
    amp_v[...] = as_col(jnp.sqrt(resid * SAMPLE_REF / ss2))
    last_out = pltpu.make_async_copy(amp_v, amp_hbm, out_sem.at[2])
    last_out.start()
    for t in range(ITERS):
        rows_wait(rbuf, t, nblk - 1, rs_sem)
    for h in range(ITERS - 1):
        rows_wait(sbuf, h, nblk - 1, ss_sem)
        rows_wait(pbuf, h, nz - 1, ps_sem)
        for k in range(NCH):
            pltpu.make_async_copy(low_v.at[h, k], low_v.at[h, k], ls_sem.at[h, k]).wait()
            pltpu.make_async_copy(low_v.at[h, k], low_v.at[h, k], qs_sem.at[h, k]).wait()
    for copy in outs:
        copy.wait()
    last_out.wait()


def shards(nx, ny, nz, ld_rows, block_first, beta_hat, psi, noise, sample_size):
    snps = ld_rows.shape[0]
    pheno = beta_hat.shape[0]
    f32, bf16 = jnp.float32, jnp.bfloat16
    V, dma = pltpu.VMEM, pltpu.SemaphoreType.DMA
    h = ITERS - 1
    nblk = nx * ny * 2
    u, v, amp = pl.pallas_call(
        functools.partial(kernel, nx, ny, nz, snps),
        out_shape=(
            jax.ShapeDtypeStruct((pheno, snps), f32),
            jax.ShapeDtypeStruct((pheno, snps), f32),
            jax.ShapeDtypeStruct((pheno, LANES), f32),
        ),
        in_specs=[pl.BlockSpec(memory_space=pl.ANY)] * 6,
        out_specs=(pl.BlockSpec(memory_space=pl.ANY),) * 3,
        scratch_shapes=[
            V((snps, snps), bf16), pltpu.SMEM((snps,), jnp.int32), V((pheno, snps), f32), V((pheno, snps), f32),
            V((ITERS, pheno, snps), bf16), V((1, pheno), jnp.int32),
            V((snps, snps), bf16), V((snps, snps), bf16), V((NCH, CH, CH), bf16), V((NCH, CH, CH), bf16),
            V((pheno, snps), f32), V((h, NCH, pheno, CH), bf16), V((h, NCH, pheno, CH), bf16),
            V((h, NCH, pheno, CH), bf16), V((pheno, snps), f32), V((pheno, snps), f32), V((pheno, snps), f32),
            V((pheno, snps), f32), V((pheno, snps), f32), V((pheno, LANES), f32),
            V((ITERS, nblk, LANES), f32), V((h, nblk, LANES), f32), V((h, nz, LANES), f32),
            dma((6,)), dma((3,)), dma((ITERS,)), dma((ITERS,)), dma((h,)), dma((h,)), dma((h,)), dma((h,)),
            dma((h, NCH)), dma((h, NCH)), dma((h, NCH)), dma((h, NCH)),
        ],
        compiler_params=pltpu.CompilerParams(collective_id=0, has_side_effects=True),
        name="shrinkage",
    )(ld_rows, block_first, beta_hat, psi, noise, sample_size.reshape(1, pheno))
    return u + amp[:, :1] * v


def solution(mesh):
    in_specs = (
        P("blk", None),
        P("blk"),
        P("phe", "blk"),
        P("phe", "blk"),
        P(None, "phe", "blk"),
        P("phe"),
    )
    body = functools.partial(shards, 4, mesh.shape["blk"] // 8, mesh.shape["phe"])
    return jax.shard_map(body, mesh=mesh, in_specs=in_specs, out_specs=P("phe", "blk"), check_vma=False)
```

```python
import functools

import jax
import jax.numpy as jnp
from jax import lax
from jax.experimental import pallas as pl
from jax.experimental.pallas import tpu as pltpu
from jax.sharding import PartitionSpec as P

ITERS = 3
TINY = 1e-06
SAMPLE_REF = 20000.0
MESH = pl.DeviceIdType.MESH
LANES = 128
NB = 8
CH = 256
NCH = 4
F32 = jnp.float32
BF16 = jnp.bfloat16
EARLY = True


def peer_offsets(nx, ny):
    def hops(d):
        dx, dy, dc = d
        return min(dx, nx - dx) + min(dy, ny - dy) + 0.2 * dc

    every = [(dx, dy, dc) for dx in range(nx) for dy in range(ny) for dc in range(2)]
    return sorted([d for d in every if d != (0, 0, 0)], key=lambda d: -hops(d))


def kernel(
    nx, ny, nz, snps,
    ld_hbm, bf_hbm, bfr_hbm, bh_hbm, psi_hbm, nz_hbm, ss_hbm,
    out_ref,
    ld_v, bf_s, bf_v, bh_v, psi_v, nz_v, ss_v,
    rt_m, x_v, acc_v, tail_v, beta_v, sh_v, u_v, v_v,
    low_v, lowl_v, lowr_v, t_v, tl_v, tr_v, psil_v, psir_v, nzl_v, nzr_v, shl_v, shr_v,
    rbuf, sbuf, pbuf,
    in_sem, rs_sem, rr_sem, ss_sem, sr_sem, ps_sem, pr_sem,
    ls_sem, lr_sem, qs_sem, qr_sem, ts_sem, tr_sem, ws_sem, wr_sem, hs_sem, hr_sem,
):
    nblk = nx * ny * 2
    me = lax.axis_index("blk")
    mz = lax.axis_index("phe")
    mx, my, mc = me // (2 * ny), (me // 2) % ny, me % 2
    offsets = peer_offsets(nx, ny)
    right_peer = (me + 1) % nblk
    left_peer = (me + nblk - 1) % nblk
    nsnp = float(snps * nblk)

    def blk_of(d):
        dx, dy, dc = d
        return ((mx + dx) % nx) * (2 * ny) + ((my + dy) % ny) * 2 + (mc + dc) % 2

    barrier = pltpu.get_barrier_semaphore()
    for d in offsets:
        pl.semaphore_signal(barrier, inc=1, device_id={"blk": blk_of(d)}, device_id_type=MESH)
    for dz in range(1, nz):
        pl.semaphore_signal(barrier, inc=1, device_id={"phe": (mz + dz) % nz}, device_id_type=MESH)

    loads = [
        pltpu.make_async_copy(bh_hbm, bh_v, in_sem.at[0]),
        pltpu.make_async_copy(psi_hbm, psi_v, in_sem.at[1]),
        pltpu.make_async_copy(nz_hbm, nz_v, in_sem.at[2]),
        pltpu.make_async_copy(bf_hbm, bf_s, in_sem.at[3]),
        pltpu.make_async_copy(bfr_hbm, bf_v, in_sem.at[4]),
        pltpu.make_async_copy(ss_hbm, ss_v, in_sem.at[5]),
        pltpu.make_async_copy(ld_hbm, ld_v, in_sem.at[6]),
    ]
    for copy in loads:
        copy.start()

    def cols(k):
        return slice(k * LANES, (k + 1) * LANES)

    def as_row(first, second):
        both = jnp.concatenate([first, second], axis=0)
        return jnp.sum(both.T, axis=0, keepdims=True)

    def as_col(row):
        return jnp.broadcast_to(row, (LANES, LANES)).T[:64]

    def remote(src, dst, ssem, rsem, who):
        return pltpu.make_async_remote_copy(src, dst, ssem, rsem, device_id=who, device_id_type=MESH)

    def bytes_wait(ref, sem):
        pltpu.make_async_copy(ref, ref, sem).wait()

    def resid_start(t, row):
        rbuf[t, pl.ds(me, 1)] = row
        for d in offsets:
            slot = rbuf.at[t, pl.ds(me, 1)]
            remote(slot, slot, rs_sem.at[t], rr_sem.at[t], {"blk": blk_of(d)}).start()

    def resid_finish(t):
        bytes_wait(rbuf.at[t, pl.ds(0, nblk - 1)], rr_sem.at[t])
        return jnp.sum(rbuf[t], axis=0, keepdims=True) / nsnp + TINY

    def scale_start(h, rows):
        sbuf[h, pl.ds(2 * me, 2)] = rows
        for d in offsets:
            slot = sbuf.at[h, pl.ds(2 * me, 2)]
            remote(slot, slot, ss_sem.at[h], sr_sem.at[h], {"blk": blk_of(d)}).start()

    def scale_finish(h, amp):
        bytes_wait(sbuf.at[h, pl.ds(0, 2 * nblk - 2)], sr_sem.at[h])
        both = jnp.sum(sbuf[h].reshape(nblk, 2, LANES), axis=0)
        c01, c2 = both[0:1], both[1:2]
        c1 = pltpu.roll(c01, 64, axis=1)
        lane = lax.broadcasted_iota(jnp.int32, (1, LANES), 1)
        total = jnp.where(lane < 64, jnp.maximum(c01 + 2.0 * amp * c1 + amp * amp * c2, 0.0), 0.0)
        mine = jnp.sum(total, axis=1, keepdims=True)
        pbuf[h, pl.ds(mz, 1)] = jnp.broadcast_to(mine, (1, LANES))
        for dz in range(1, nz):
            slot = pbuf.at[h, pl.ds(mz, 1)]
            remote(slot, slot, ps_sem.at[h], pr_sem.at[h], {"phe": (mz + dz) % nz}).start()
        return total

    def phi_finish(h, total):
        bytes_wait(pbuf.at[h, pl.ds(0, nz - 1)], pr_sem.at[h])
        pooled = jnp.sum(pbuf[h], axis=0, keepdims=True) / (nsnp * (64 * nz)) + TINY
        return as_col((total / nsnp + TINY + pooled) / 2.0)

    def coefficients(t, value):
        zero = jnp.zeros((64, LANES), F32)
        c0, c1, c2 = zero, zero, zero
        for k in range(NB):
            s = sh_v[:, cols(k)]
            w = s * s / psi_v[:, cols(k)]
            x = value(k)
            n = nz_v[t, :, cols(k)].astype(F32)
            c0 = c0 + w * x * x
            c1 = c1 + w * x * n
            c2 = c2 + w * n * n
        return jnp.concatenate([as_row(c0, c1), as_row(c2, zero)], axis=0)

    def half(k):
        return k // 2, slice((k % 2) * LANES, (k % 2 + 1) * LANES)

    zero = jnp.zeros((64, LANES), F32)
    loads[0].wait()
    acc = zero
    for k in range(NB):
        b = bh_v[:, cols(k)]
        acc = acc + b * b
    row0 = as_row(acc, zero)
    loads[1].wait()
    loads[2].wait()
    for k in range(NB):
        psi = psi_v[:, cols(k)]
        sh_v[:, cols(k)] = psi / (psi + TINY)
    coef0 = coefficients(0, lambda k: bh_v[:, cols(k)])
    pl.semaphore_wait(barrier, nblk - 1 + nz - 1)
    resid_start(0, row0)
    scale_start(0, coef0)

    early = [
        remote(psi_v, psil_v, ws_sem.at[0], wr_sem.at[0], {"blk": right_peer}),
        remote(psi_v, psir_v, ws_sem.at[1], wr_sem.at[1], {"blk": left_peer}),
        remote(nz_v.at[1], nzl_v, ws_sem.at[2], wr_sem.at[2], {"blk": right_peer}),
        remote(nz_v.at[1], nzr_v, ws_sem.at[3], wr_sem.at[3], {"blk": left_peer}),
    ]
    if EARLY:
        for copy in early:
            copy.start()

    for copy in loads[3:]:
        copy.wait()
    base = me * snps
    sub = lax.broadcasted_iota(jnp.int32, (LANES, snps), 0)
    for i in range(NB):
        rows = slice(i * LANES, (i + 1) * LANES)
        first = bf_s[i * LANES]
        last = bf_s[i * LANES + LANES - 1]
        tile = ld_v[rows, :].astype(F32)
        ra = pltpu.roll(tile, first & (snps - 1), axis=1)
        rb = pltpu.roll(tile, last & (snps - 1), axis=1)
        split = jnp.where(last == first, LANES, last - base - i * LANES)
        rt_m[:, rows] = jnp.where(sub >= split, rb, ra).T.astype(BF16)
    begin = bf_s[0]
    end = bf_s[snps - 1]
    from_left = jnp.where(begin < base, begin & (snps - 1), snps)
    to_right = end & (snps - 1)
    lane = lax.broadcasted_iota(jnp.int32, (64, LANES), 1)

    ss = ss_v[...].astype(F32)
    ss2 = jnp.concatenate([ss, ss], axis=1)

    amp_row = jnp.sqrt(resid_finish(0) * SAMPLE_REF / ss2)
    amp = as_col(amp_row)
    for k in range(NB):
        b = sh_v[:, cols(k)] * (bh_v[:, cols(k)] + amp * nz_v[0, :, cols(k)].astype(F32))
        beta_v[:, cols(k)] = b
        c, w = half(k)
        low_v[c, :, w] = b.astype(BF16)
        x_v[0:64, cols(k)] = b.astype(BF16)
        x_v[64:128, cols(k)] = jnp.where(lane + k * LANES < from_left, b, 0.0).astype(BF16)
        x_v[128:192, cols(k)] = jnp.where(lane + k * LANES >= to_right, b, 0.0).astype(BF16)
    halo = []
    for k in range(NCH):
        kr, kl = NCH - 1 - k, k
        a = remote(low_v.at[kr], lowl_v.at[kr], ls_sem.at[kr], lr_sem.at[kr], {"blk": right_peer})
        b = remote(low_v.at[kl], lowr_v.at[kl], qs_sem.at[kl], qr_sem.at[kl], {"blk": left_peer})
        a.start()
        b.start()
        halo.append((kr, kl, a, b))
    if not EARLY:
        for copy in early:
            copy.start()
    total = scale_finish(0, amp_row)
    acc_v[...] = jnp.dot(x_v[...], rt_m[...], preferred_element_type=F32)
    for kr, kl, a, b in halo:
        a.wait_recv()
        q = lax.broadcasted_iota(jnp.int32, (64, CH), 1)
        x = jnp.where(q + kr * CH >= from_left, lowl_v[kr].astype(F32), 0.0).astype(BF16)
        upto = slice(0, (kr + 1) * CH)
        acc_v[64:128, upto] += jnp.dot(x, rt_m[kr * CH:(kr + 1) * CH, upto], preferred_element_type=F32)
        b.wait_recv()
        x = jnp.where(q + kl * CH < to_right, lowr_v[kl].astype(F32), 0.0).astype(BF16)
        upto = slice(kl * CH, snps)
        acc_v[128:192, upto] += jnp.dot(x, rt_m[kl * CH:(kl + 1) * CH, upto], preferred_element_type=F32)

    def gradient(k):
        first = bf_v[:, cols(k)]
        applied = jnp.where(
            first < base, acc_v[64:128, cols(k)],
            jnp.where(first == end, acc_v[128:192, cols(k)], acc_v[0:64, cols(k)]),
        )
        return bh_v[:, cols(k)] - applied

    racc = zero
    for k in range(NB):
        g = gradient(k)
        racc = racc + g * g
        c, w = half(k)
        t_v[c, :, w] = beta_v[:, cols(k)] + g
    resid_start(1, as_row(racc, zero))

    sums = []
    for k in range(NCH):
        kr, kl = NCH - 1 - k, k
        sums.append(remote(t_v.at[kr], tl_v.at[kr], ts_sem.at[kr], tr_sem.at[kr], {"blk": right_peer}))
        sums.append(remote(t_v.at[kl], tr_v.at[kl], hs_sem.at[kl], hr_sem.at[kl], {"blk": left_peer}))
    for copy in sums:
        copy.start()

    phi = phi_finish(0, total)
    for k in range(NB):
        psi = psi_v[:, cols(k)]
        sh_v[:, cols(k)] = psi / (psi + phi)

    def t_of(k):
        c, w = half(k)
        return t_v[c, :, w]

    scale_start(1, coefficients(1, t_of))
    for copy in early:
        copy.wait_recv()
    for k in range(NB):
        psi = psil_v[:, cols(k)]
        shl_v[:, cols(k)] = psi / (psi + phi)
        psi = psir_v[:, cols(k)]
        shr_v[:, cols(k)] = psi / (psi + phi)

    amp_row = jnp.sqrt(resid_finish(1) * SAMPLE_REF / ss2)
    amp = as_col(amp_row)
    for copy in sums:
        copy.wait_recv()
    for k in range(NB):
        c, w = half(k)
        b = sh_v[:, cols(k)] * (t_v[c, :, w] + amp * nz_v[1, :, cols(k)].astype(F32))
        bl = shl_v[:, cols(k)] * (tl_v[c, :, w] + amp * nzl_v[:, cols(k)].astype(F32))
        br = shr_v[:, cols(k)] * (tr_v[c, :, w] + amp * nzr_v[:, cols(k)].astype(F32))
        beta_v[:, cols(k)] = b
        x_v[0:64, cols(k)] = b.astype(BF16)
        x_v[64:128, cols(k)] = jnp.where(lane + k * LANES < from_left, b, bl).astype(BF16)
        x_v[128:192, cols(k)] = jnp.where(lane + k * LANES >= to_right, b, br).astype(BF16)
    acc_v[...] = jnp.dot(x_v[...], rt_m[...], preferred_element_type=F32)
    racc = zero
    for k in range(NB):
        g = gradient(k)
        racc = racc + g * g
        tail_v[:, cols(k)] = beta_v[:, cols(k)] + g
    resid_start(2, as_row(racc, zero))
    phi = phi_finish(1, scale_finish(1, amp_row))
    for k in range(NB):
        psi = psi_v[:, cols(k)]
        shrink = psi / (psi + phi)
        u_v[:, cols(k)] = shrink * tail_v[:, cols(k)]
        v_v[:, cols(k)] = shrink * nz_v[2, :, cols(k)].astype(F32)

    for t in range(ITERS):
        bytes_wait(rbuf.at[t, pl.ds(0, nblk - 1)], rs_sem.at[t])
    for h in range(ITERS - 1):
        bytes_wait(sbuf.at[h, pl.ds(0, 2 * nblk - 2)], ss_sem.at[h])
        bytes_wait(pbuf.at[h, pl.ds(0, nz - 1)], ps_sem.at[h])
    for copy in early + sums:
        copy.wait_send()
    for kr, kl, a, b in halo:
        a.wait_send()
        b.wait_send()
    amp = as_col(jnp.sqrt(resid_finish(2) * SAMPLE_REF / ss2))
    for k in range(NB):
        out_ref[:, cols(k)] = u_v[:, cols(k)] + amp * v_v[:, cols(k)]


def shards(nx, ny, nz, ld_rows, block_first, beta_hat, psi, noise, sample_size):
    snps = ld_rows.shape[0]
    pheno = beta_hat.shape[0]
    V, dma = pltpu.VMEM, pltpu.SemaphoreType.DMA
    h = ITERS - 1
    nblk = nx * ny * 2
    wide = V((pheno, snps), F32)
    chunks = V((NCH, pheno, CH), F32)
    low = V((NCH, pheno, CH), BF16)
    thin = V((pheno, snps), BF16)
    four = dma((NCH,))
    return pl.pallas_call(
        functools.partial(kernel, nx, ny, nz, snps),
        out_shape=jax.ShapeDtypeStruct((pheno, snps), F32),
        in_specs=[pl.BlockSpec(memory_space=pl.ANY)] * 7,
        out_specs=pl.BlockSpec(memory_space=pltpu.VMEM),
        scratch_shapes=[
            V((snps, snps), BF16), pltpu.SMEM((snps,), jnp.int32), V((1, snps), jnp.int32), wide, wide,
            V((ITERS, pheno, snps), BF16), V((1, pheno), jnp.int32),
            V((snps, snps), BF16), V((3 * pheno, snps), BF16), V((3 * pheno, snps), F32), wide, wide, wide, wide, wide,
            low, low, low, chunks, chunks, chunks, wide, wide, thin, thin, wide, wide,
            V((ITERS, nblk, LANES), F32), V((h, 2 * nblk, LANES), F32), V((h, nz, LANES), F32),
            dma((7,)), dma((ITERS,)), dma((ITERS,)), dma((h,)), dma((h,)), dma((h,)), dma((h,)),
            four, four, four, four, four, four, four, four, four, four,
        ],
        compiler_params=pltpu.CompilerParams(collective_id=0, has_side_effects=True),
        name="shrinkage",
    )(ld_rows, block_first, block_first.reshape(1, snps), beta_hat, psi, noise, sample_size.reshape(1, pheno))


def solution(mesh):
    in_specs = (
        P("blk", None),
        P("blk"),
        P("phe", "blk"),
        P("phe", "blk"),
        P(None, "phe", "blk"),
        P("phe"),
    )
    body = functools.partial(shards, 4, mesh.shape["blk"] // 8, mesh.shape["phe"])
    return jax.shard_map(body, mesh=mesh, in_specs=in_specs, out_specs=P("phe", "blk"), check_vma=False)
```

```python
import functools

import jax
import jax.numpy as jnp
from jax import lax
from jax.experimental import pallas as pl
from jax.experimental.pallas import tpu as pltpu
from jax.sharding import PartitionSpec as P

ITERS = 3
TINY = 1e-06
SAMPLE_REF = 20000.0
MESH = pl.DeviceIdType.MESH
LANES = 128
NB = 8
CH = 256
NCH = 4
F32 = jnp.float32
BF16 = jnp.bfloat16


def peer_offsets(nx, ny):
    def hops(d):
        dx, dy, dc = d
        return min(dx, nx - dx) + min(dy, ny - dy) + 0.2 * dc

    every = [(dx, dy, dc) for dx in range(nx) for dy in range(ny) for dc in range(2)]
    return sorted([d for d in every if d != (0, 0, 0)], key=lambda d: -hops(d))


def kernel(
    nx, ny, nz, snps,
    ld_hbm, bf_hbm, bfr_hbm, bh_hbm, psi_hbm, nz_hbm, ss_hbm,
    out_ref,
    ld_v, bf_s, bf_v, bh_v, psi_v, nz_v, ss_v,
    rt_m, x_v, acc_v, tail_v, beta_v, sh_v, u_v, v_v,
    low_v, lowl_v, lowr_v, t_v, tl_v, tr_v, psil_v, psir_v, nzl_v, nzr_v, shl_v, shr_v,
    rbuf, sbuf, cbuf, pair_v, pbuf,
    in_sem, rs_sem, rr_sem, ss_sem, sr_sem, ps_sem, pr_sem,
    ls_sem, lr_sem, qs_sem, qr_sem, ts_sem, tr_sem, ws_sem, wr_sem, hs_sem, hr_sem, cs_sem, go_sem,
):
    nblk = nx * ny * 2
    me = lax.axis_index("blk")
    mz = lax.axis_index("phe")
    mx, my, mc = me // (2 * ny), (me // 2) % ny, me % 2
    offsets = peer_offsets(nx, ny)
    right_peer = (me + 1) % nblk
    left_peer = (me + nblk - 1) % nblk
    nsnp = float(snps * nblk)

    def blk_of(d):
        dx, dy, dc = d
        return ((mx + dx) % nx) * (2 * ny) + ((my + dy) % ny) * 2 + (mc + dc) % 2

    barrier = pltpu.get_barrier_semaphore()
    partner = me + 1 - 2 * mc
    for d in offsets:
        if d[2] == 0:
            chip = blk_of(d) // 2
            pl.semaphore_signal(barrier, inc=1, device_id={"blk": 2 * chip + 1}, device_id_type=MESH)

    @pl.when(mc == 0)
    def _():
        pl.semaphore_signal(barrier, inc=1, device_id={"blk": partner}, device_id_type=MESH)

    loads = [
        pltpu.make_async_copy(bh_hbm, bh_v, in_sem.at[0]),
        pltpu.make_async_copy(psi_hbm, psi_v, in_sem.at[1]),
        pltpu.make_async_copy(nz_hbm, nz_v, in_sem.at[2]),
        pltpu.make_async_copy(bf_hbm, bf_s, in_sem.at[3]),
        pltpu.make_async_copy(bfr_hbm, bf_v, in_sem.at[4]),
        pltpu.make_async_copy(ss_hbm, ss_v, in_sem.at[5]),
        pltpu.make_async_copy(ld_hbm, ld_v, in_sem.at[6]),
    ]
    for copy in loads:
        copy.start()

    def cols(k):
        return slice(k * LANES, (k + 1) * LANES)

    def as_row(first, second):
        both = jnp.concatenate([first, second], axis=0)
        return jnp.sum(both.T, axis=0, keepdims=True)

    def as_col(row):
        return jnp.broadcast_to(row, (LANES, LANES)).T[:64]

    def remote(src, dst, ssem, rsem, who):
        return pltpu.make_async_remote_copy(src, dst, ssem, rsem, device_id=who, device_id_type=MESH)

    def bytes_wait(ref, sem):
        pltpu.make_async_copy(ref, ref, sem).wait()

    def resid_start(t, row):
        rbuf[t, pl.ds(me, 1)] = row
        for d in offsets:
            slot = rbuf.at[t, pl.ds(me, 1)]
            remote(slot, slot, rs_sem.at[t], rr_sem.at[t], {"blk": blk_of(d)}).start()

    def resid_finish(t):
        bytes_wait(rbuf.at[t, pl.ds(0, nblk - 1)], rr_sem.at[t])
        return jnp.sum(rbuf[t], axis=0, keepdims=True) / nsnp + TINY

    def scale_start(rows):
        sbuf[pl.ds(2 * me, 2)] = rows
        for d in offsets:
            slot = sbuf.at[pl.ds(2 * me, 2)]
            remote(slot, slot, ss_sem.at[0], sr_sem.at[0], {"blk": blk_of(d)}).start()

    def paired_start(rows):
        pair_v[0:2] = rows
        swap = remote(pair_v.at[0:2], pair_v.at[8:10], cs_sem.at[0], cs_sem.at[1], {"blk": partner})
        swap.start()
        swap.wait()
        mine = me // 2
        cbuf[pl.ds(2 * mine, 2)] = rows + pair_v[8:10]
        slot = cbuf.at[pl.ds(2 * mine, 2)]

        def send(chips):
            for dx, dy in chips:
                chip = blk_of((dx, dy, 0)) // 2
                for c in range(2):
                    remote(slot, slot, ss_sem.at[1], sr_sem.at[1], {"blk": 2 * chip + c}).start()

        chips = [(dx, dy) for dx, dy, dc in offsets if dc == 0]
        ups = [d for d in chips if d[1] < ny // 2]
        downs = [d for d in chips if d[1] >= ny // 2]

        @pl.when(mc == 0)
        def _():
            send(ups)

        @pl.when(mc == 1)
        def _():
            send(downs)

        return 2 * len(ups), 2 * len(downs)

    def scale_finish(h, amp):
        if h == 0:
            bytes_wait(sbuf.at[pl.ds(0, 2 * nblk - 2)], sr_sem.at[h])
            both = jnp.sum(sbuf[...].reshape(nblk, 2, LANES), axis=0)
        else:
            bytes_wait(cbuf.at[pl.ds(0, nblk - 2)], sr_sem.at[h])
            both = jnp.sum(cbuf[...].reshape(nblk // 2, 2, LANES), axis=0)
        c01, c2 = both[0:1], both[1:2]
        c1 = pltpu.roll(c01, 64, axis=1)
        lane = lax.broadcasted_iota(jnp.int32, (1, LANES), 1)
        total = jnp.where(lane < 64, jnp.maximum(c01 + 2.0 * amp * c1 + amp * amp * c2, 0.0), 0.0)
        mine = jnp.sum(total, axis=1, keepdims=True)
        pbuf[h, pl.ds(mz, 1)] = jnp.broadcast_to(mine, (1, LANES))
        for dz in range(1, nz):
            slot = pbuf.at[h, pl.ds(mz, 1)]
            remote(slot, slot, ps_sem.at[h], pr_sem.at[h], {"phe": (mz + dz) % nz}).start()
        return total

    def phi_finish(h, total):
        bytes_wait(pbuf.at[h, pl.ds(0, nz - 1)], pr_sem.at[h])
        pooled = jnp.sum(pbuf[h], axis=0, keepdims=True) / (nsnp * (64 * nz)) + TINY
        return as_col((total / nsnp + TINY + pooled) / 2.0)

    def coefficients(t, value):
        zero = jnp.zeros((64, LANES), F32)
        c0, c1, c2 = zero, zero, zero
        for k in range(NB):
            s = sh_v[:, cols(k)]
            w = s * s / psi_v[:, cols(k)]
            x = value(k)
            n = nz_v[t, :, cols(k)].astype(F32)
            c0 = c0 + w * x * x
            c1 = c1 + w * x * n
            c2 = c2 + w * n * n
        return jnp.concatenate([as_row(c0, c1), as_row(c2, zero)], axis=0)

    def half(k):
        return k // 2, slice((k % 2) * LANES, (k % 2 + 1) * LANES)

    zero = jnp.zeros((64, LANES), F32)
    loads[0].wait()
    acc = zero
    for k in range(NB):
        b = bh_v[:, cols(k)]
        acc = acc + b * b
    row0 = as_row(acc, zero)
    loads[1].wait()
    loads[2].wait()
    for k in range(NB):
        psi = psi_v[:, cols(k)]
        sh_v[:, cols(k)] = psi / (psi + TINY)
    coef0 = coefficients(0, lambda k: bh_v[:, cols(k)])
    @pl.when(mc == 1)
    def _():
        pl.semaphore_wait(barrier, nblk - 1)
        pl.semaphore_signal(go_sem, inc=1, device_id={"blk": partner}, device_id_type=MESH)

    @pl.when(mc == 0)
    def _():
        pl.semaphore_wait(go_sem, 1)

    resid_start(0, row0)

    @pl.when(mc == 0)
    def _():
        for dz in range(1, nz):
            pl.semaphore_signal(barrier, inc=1, device_id={"phe": (mz + dz) % nz}, device_id_type=MESH)

    scale_start(coef0)

    early = [
        remote(psi_v, psil_v, ws_sem.at[0], wr_sem.at[0], {"blk": right_peer}),
        remote(psi_v, psir_v, ws_sem.at[1], wr_sem.at[1], {"blk": left_peer}),
        remote(nz_v.at[1], nzl_v, ws_sem.at[2], wr_sem.at[2], {"blk": right_peer}),
        remote(nz_v.at[1], nzr_v, ws_sem.at[3], wr_sem.at[3], {"blk": left_peer}),
    ]
    for copy in early[2:]:
        copy.start()

    for copy in loads[3:]:
        copy.wait()
    base = me * snps
    sub = lax.broadcasted_iota(jnp.int32, (LANES, snps), 0)
    for i in range(NB):
        rows = slice(i * LANES, (i + 1) * LANES)
        first = bf_s[i * LANES]
        last = bf_s[i * LANES + LANES - 1]
        tile = ld_v[rows, :].astype(F32)
        ra = pltpu.roll(tile, first & (snps - 1), axis=1)
        rb = pltpu.roll(tile, last & (snps - 1), axis=1)
        split = jnp.where(last == first, LANES, last - base - i * LANES)
        rt_m[:, rows] = jnp.where(sub >= split, rb, ra).T.astype(BF16)
    begin = bf_s[0]
    end = bf_s[snps - 1]
    from_left = jnp.where(begin < base, begin & (snps - 1), snps)
    to_right = end & (snps - 1)
    lane = lax.broadcasted_iota(jnp.int32, (64, LANES), 1)

    ss = ss_v[...].astype(F32)
    ss2 = jnp.concatenate([ss, ss], axis=1)

    amp_row = jnp.sqrt(resid_finish(0) * SAMPLE_REF / ss2)
    amp = as_col(amp_row)
    for k in range(NB):
        b = sh_v[:, cols(k)] * (bh_v[:, cols(k)] + amp * nz_v[0, :, cols(k)].astype(F32))
        beta_v[:, cols(k)] = b
        c, w = half(k)
        low_v[c, :, w] = b.astype(BF16)
        x_v[0:64, cols(k)] = b.astype(BF16)
        x_v[64:128, cols(k)] = jnp.where(lane + k * LANES < from_left, b, 0.0).astype(BF16)
        x_v[128:192, cols(k)] = jnp.where(lane + k * LANES >= to_right, b, 0.0).astype(BF16)
    halo = []
    for k in range(NCH):
        kr, kl = NCH - 1 - k, k
        a = remote(low_v.at[kr], lowl_v.at[kr], ls_sem.at[kr], lr_sem.at[kr], {"blk": right_peer})
        b = remote(low_v.at[kl], lowr_v.at[kl], qs_sem.at[kl], qr_sem.at[kl], {"blk": left_peer})
        a.start()
        b.start()
        halo.append((kr, kl, a, b))
    for copy in early[:2]:
        copy.start()

    @pl.when(mc == 0)
    def _():
        pl.semaphore_wait(barrier, nz - 1)
        pl.semaphore_signal(go_sem, inc=1, device_id={"blk": partner}, device_id_type=MESH)

    @pl.when(mc == 1)
    def _():
        pl.semaphore_wait(go_sem, 1)

    total = scale_finish(0, amp_row)
    acc_v[...] = jnp.dot(x_v[...], rt_m[...], preferred_element_type=F32)
    for kr, kl, a, b in halo:
        a.wait_recv()
        q = lax.broadcasted_iota(jnp.int32, (64, CH), 1)
        x = jnp.where(q + kr * CH >= from_left, lowl_v[kr].astype(F32), 0.0).astype(BF16)
        upto = slice(0, (kr + 1) * CH)
        acc_v[64:128, upto] += jnp.dot(x, rt_m[kr * CH:(kr + 1) * CH, upto], preferred_element_type=F32)
        b.wait_recv()
        x = jnp.where(q + kl * CH < to_right, lowr_v[kl].astype(F32), 0.0).astype(BF16)
        upto = slice(kl * CH, snps)
        acc_v[128:192, upto] += jnp.dot(x, rt_m[kl * CH:(kl + 1) * CH, upto], preferred_element_type=F32)

    def gradient(k):
        first = bf_v[:, cols(k)]
        applied = jnp.where(
            first < base, acc_v[64:128, cols(k)],
            jnp.where(first == end, acc_v[128:192, cols(k)], acc_v[0:64, cols(k)]),
        )
        return bh_v[:, cols(k)] - applied

    racc = zero
    for k in range(NB):
        g = gradient(k)
        racc = racc + g * g
        c, w = half(k)
        t_v[c, :, w] = beta_v[:, cols(k)] + g
    resid_start(1, as_row(racc, zero))

    sums = []
    for k in range(NCH):
        kr, kl = NCH - 1 - k, k
        sums.append(remote(t_v.at[kr], tl_v.at[kr], ts_sem.at[kr], tr_sem.at[kr], {"blk": right_peer}))
        sums.append(remote(t_v.at[kl], tr_v.at[kl], hs_sem.at[kl], hr_sem.at[kl], {"blk": left_peer}))
    for copy in sums:
        copy.start()

    phi = phi_finish(0, total)
    for k in range(NB):
        psi = psi_v[:, cols(k)]
        sh_v[:, cols(k)] = psi / (psi + phi)

    def t_of(k):
        c, w = half(k)
        return t_v[c, :, w]

    n_ups, n_downs = paired_start(coefficients(1, t_of))
    for copy in early:
        copy.wait_recv()
    for k in range(NB):
        psi = psil_v[:, cols(k)]
        shl_v[:, cols(k)] = psi / (psi + phi)
        psi = psir_v[:, cols(k)]
        shr_v[:, cols(k)] = psi / (psi + phi)

    amp_row = jnp.sqrt(resid_finish(1) * SAMPLE_REF / ss2)
    amp = as_col(amp_row)
    for copy in sums:
        copy.wait_recv()
    for k in range(NB):
        c, w = half(k)
        b = sh_v[:, cols(k)] * (t_v[c, :, w] + amp * nz_v[1, :, cols(k)].astype(F32))
        bl = shl_v[:, cols(k)] * (tl_v[c, :, w] + amp * nzl_v[:, cols(k)].astype(F32))
        br = shr_v[:, cols(k)] * (tr_v[c, :, w] + amp * nzr_v[:, cols(k)].astype(F32))
        beta_v[:, cols(k)] = b
        x_v[0:64, cols(k)] = b.astype(BF16)
        x_v[64:128, cols(k)] = jnp.where(lane + k * LANES < from_left, b, bl).astype(BF16)
        x_v[128:192, cols(k)] = jnp.where(lane + k * LANES >= to_right, b, br).astype(BF16)
    acc_v[...] = jnp.dot(x_v[...], rt_m[...], preferred_element_type=F32)
    racc = zero
    for k in range(NB):
        g = gradient(k)
        racc = racc + g * g
        tail_v[:, cols(k)] = beta_v[:, cols(k)] + g
    resid_start(2, as_row(racc, zero))
    phi = phi_finish(1, scale_finish(1, amp_row))
    for k in range(NB):
        psi = psi_v[:, cols(k)]
        shrink = psi / (psi + phi)
        u_v[:, cols(k)] = shrink * tail_v[:, cols(k)]
        v_v[:, cols(k)] = shrink * nz_v[2, :, cols(k)].astype(F32)

    for t in range(ITERS):
        bytes_wait(rbuf.at[t, pl.ds(0, nblk - 1)], rs_sem.at[t])
    for h in range(ITERS - 1):
        bytes_wait(pbuf.at[h, pl.ds(0, nz - 1)], ps_sem.at[h])
    bytes_wait(sbuf.at[pl.ds(0, 2 * nblk - 2)], ss_sem.at[0])

    @pl.when(mc == 0)
    def _():
        bytes_wait(sbuf.at[pl.ds(0, 2 * n_ups)], ss_sem.at[1])

    @pl.when(mc == 1)
    def _():
        bytes_wait(sbuf.at[pl.ds(0, 2 * n_downs)], ss_sem.at[1])

    for copy in early + sums:
        copy.wait_send()
    for kr, kl, a, b in halo:
        a.wait_send()
        b.wait_send()
    amp = as_col(jnp.sqrt(resid_finish(2) * SAMPLE_REF / ss2))
    for k in range(NB):
        out_ref[:, cols(k)] = u_v[:, cols(k)] + amp * v_v[:, cols(k)]


def shards(nx, ny, nz, ld_rows, block_first, beta_hat, psi, noise, sample_size):
    snps = ld_rows.shape[0]
    pheno = beta_hat.shape[0]
    V, dma = pltpu.VMEM, pltpu.SemaphoreType.DMA
    h = ITERS - 1
    nblk = nx * ny * 2
    wide = V((pheno, snps), F32)
    chunks = V((NCH, pheno, CH), F32)
    low = V((NCH, pheno, CH), BF16)
    thin = V((pheno, snps), BF16)
    four = dma((NCH,))
    arrays = (ld_rows, block_first, block_first.reshape(1, snps), beta_hat, psi, noise, sample_size.reshape(1, pheno))
    return pl.pallas_call(
        functools.partial(kernel, nx, ny, nz, snps),
        out_shape=pltpu.VMEM((pheno, snps), F32),
        in_specs=[pl.BlockSpec(memory_space=pl.ANY)] * 7,
        out_specs=pl.BlockSpec(memory_space=pltpu.VMEM),
        scratch_shapes=[
            V((snps, snps), BF16), pltpu.SMEM((snps,), jnp.int32), V((1, snps), jnp.int32), wide, wide,
            V((ITERS, pheno, snps), BF16), V((1, pheno), jnp.int32),
            V((snps, snps), BF16), V((3 * pheno, snps), BF16), V((3 * pheno, snps), F32), wide, wide, wide, wide, wide,
            low, low, low, chunks, chunks, chunks, wide, wide, thin, thin, wide, wide,
            V((ITERS, nblk, LANES), F32), V((2 * nblk, LANES), F32), V((nblk, LANES), F32),
            V((16, LANES), F32), V((h, nz, LANES), F32),
            dma((7,)), dma((ITERS,)), dma((ITERS,)), dma((h,)), dma((h,)), dma((h,)), dma((h,)),
            four, four, four, four, four, four, four, four, four, four, dma((2,)), pltpu.SemaphoreType.REGULAR,
        ],
        compiler_params=pltpu.CompilerParams(collective_id=0, has_side_effects=True, vmem_limit_bytes=32 * 1024 * 1024),
        name="shrinkage",
    )(*[pltpu.with_memory_space_constraint(a, pltpu.HBM) for a in arrays])


def solution(mesh):
    in_specs = (
        P("blk", None),
        P("blk"),
        P("phe", "blk"),
        P("phe", "blk"),
        P(None, "phe", "blk"),
        P("phe"),
    )
    body = functools.partial(shards, 4, mesh.shape["blk"] // 8, mesh.shape["phe"])
    return jax.shard_map(body, mesh=mesh, in_specs=in_specs, out_specs=P("phe", "blk"), check_vma=False)
```

```python
import functools

import jax
import jax.numpy as jnp
from jax import lax
from jax.experimental import pallas as pl
from jax.experimental.pallas import tpu as pltpu
from jax.sharding import PartitionSpec as P

ITERS = 3
TINY = 1e-06
SAMPLE_REF = 20000.0
MESH = pl.DeviceIdType.MESH
LANES = 128
NB = 8
CH = 256
NCH = 4
F32 = jnp.float32
BF16 = jnp.bfloat16


def peer_offsets(nx, ny):
    def hops(d):
        dx, dy, dc = d
        return min(dx, nx - dx) + min(dy, ny - dy) + 0.2 * dc

    every = [(dx, dy, dc) for dx in range(nx) for dy in range(ny) for dc in range(2)]
    return sorted([d for d in every if d != (0, 0, 0)], key=lambda d: -hops(d))


def kernel(
    nx, ny, nz, snps,
    ld_hbm, bf_hbm, bfr_hbm, bh_hbm, psi_hbm, nz_hbm, ss_hbm,
    out_ref,
    ld_v, bf_s, bf_v, bh_v, psi_v, nz_v, ss_v,
    rt_m, x_v, acc_v, tail_v, beta_v, sh_v, u_v, v_v,
    low_v, lowl_v, lowr_v, t_v, tl_v, tr_v, psil_v, psir_v, nzl_v, nzr_v, shl_v, shr_v,
    rbuf, sbuf, pbuf, total_v,
    in_sem, rs_sem, rr_sem, ss_sem, sr_sem, ps_sem, pr_sem,
    ls_sem, lr_sem, qs_sem, qr_sem, ts_sem, tr_sem, ws_sem, wr_sem, hs_sem, hr_sem, go_sem,
):
    nblk = nx * ny * 2
    me = lax.axis_index("blk")
    mz = lax.axis_index("phe")
    mx, my, mc = me // (2 * ny), (me // 2) % ny, me % 2
    offsets = peer_offsets(nx, ny)
    right_peer = (me + 1) % nblk
    left_peer = (me + nblk - 1) % nblk
    nsnp = float(snps * nblk)

    def blk_of(d):
        dx, dy, dc = d
        return ((mx + dx) % nx) * (2 * ny) + ((my + dy) % ny) * 2 + (mc + dc) % 2

    barrier = pltpu.get_barrier_semaphore()
    partner = me + 1 - 2 * mc
    not_first = me > 0
    not_last = me < nblk - 1
    for d in offsets:
        if d[2] == 0:
            chip = blk_of(d) // 2
            pl.semaphore_signal(barrier, inc=1, device_id={"blk": 2 * chip}, device_id_type=MESH)

    @pl.when(mc == 1)
    def _():
        pl.semaphore_signal(barrier, inc=1, device_id={"blk": partner}, device_id_type=MESH)

    loads = [
        pltpu.make_async_copy(bh_hbm, bh_v, in_sem.at[0]),
        pltpu.make_async_copy(psi_hbm, psi_v, in_sem.at[1]),
        pltpu.make_async_copy(nz_hbm, nz_v, in_sem.at[2]),
        pltpu.make_async_copy(bf_hbm, bf_s, in_sem.at[3]),
        pltpu.make_async_copy(bfr_hbm, bf_v, in_sem.at[4]),
        pltpu.make_async_copy(ss_hbm, ss_v, in_sem.at[5]),
        pltpu.make_async_copy(ld_hbm, ld_v, in_sem.at[6]),
    ]
    for copy in loads:
        copy.start()

    def cols(k):
        return slice(k * LANES, (k + 1) * LANES)

    def as_row(first, second):
        both = jnp.concatenate([first, second], axis=0)
        return jnp.sum(both.T, axis=0, keepdims=True)

    def as_col(row):
        return jnp.broadcast_to(row, (LANES, LANES)).T[:64]

    def remote(src, dst, ssem, rsem, who):
        return pltpu.make_async_remote_copy(src, dst, ssem, rsem, device_id=who, device_id_type=MESH)

    def bytes_wait(ref, sem):
        pltpu.make_async_copy(ref, ref, sem).wait()

    def to_all(ref, ssem, rsem):
        for d in offsets:
            remote(ref, ref, ssem, rsem, {"blk": blk_of(d)}).start()

    def resid_start(t, row):
        rbuf[t, pl.ds(me, 1)] = row
        to_all(rbuf.at[t, pl.ds(me, 1)], rs_sem.at[t], rr_sem.at[t])

    def resid_finish(t):
        bytes_wait(rbuf.at[t, pl.ds(0, nblk - 1)], rr_sem.at[t])
        return amplitude(jnp.sum(rbuf[t], axis=0, keepdims=True))

    def amplitude(total):
        return jnp.sqrt((total / nsnp + TINY) * SAMPLE_REF / ss2)

    def scale_start(h, rows):
        sbuf[h, pl.ds(2 * me, 2)] = rows
        to_all(sbuf.at[h, pl.ds(2 * me, 2)], ss_sem.at[h], sr_sem.at[h])

    def scale_sums(h):
        bytes_wait(sbuf.at[h, pl.ds(0, 2 * nblk - 2)], sr_sem.at[h])
        return jnp.sum(sbuf[h].reshape(nblk, 2, LANES), axis=0)

    def scale_finish(h, both, amp):
        c0 = pltpu.roll(both[0:1], 64, axis=1)
        c1 = both[1:2]
        c2 = pltpu.roll(both[1:2], 64, axis=1)
        lane = lax.broadcasted_iota(jnp.int32, (1, LANES), 1)
        total = jnp.where(lane < 64, jnp.maximum(c0 + 2.0 * amp * c1 + amp * amp * c2, 0.0), 0.0)
        mine = jnp.sum(total, axis=1, keepdims=True)
        pbuf[h, pl.ds(mz, 1)] = jnp.broadcast_to(mine, (1, LANES))

        @pl.when(mc == 1)
        def _():
            slot = pbuf.at[h, pl.ds(mz, 1)]
            for blk in (partner, me):
                for dz in sorted(range(1, nz), key=lambda d: -min(d, nz - d)):
                    who = {"blk": blk, "phe": (mz + dz) % nz}
                    remote(slot, slot, ps_sem.at[h], pr_sem.at[h], who).start()

        return total

    def phi_finish(h, total):
        bytes_wait(pbuf.at[h, pl.ds(0, nz - 1)], pr_sem.at[h])
        pooled = jnp.sum(pbuf[h], axis=0, keepdims=True) / (nsnp * (64 * nz)) + TINY
        return as_col((total / nsnp + TINY + pooled) / 2.0)

    def coefficients(t, value, resid):
        zero = jnp.zeros((64, LANES), F32)
        c0, c1, c2 = zero, zero, zero
        for k in range(NB):
            s = sh_v[:, cols(k)]
            w = s * s / psi_v[:, cols(k)]
            x = value(k)
            n = nz_v[t, :, cols(k)].astype(F32)
            c0 = c0 + w * x * x
            c1 = c1 + w * x * n
            c2 = c2 + w * n * n
        return jnp.concatenate([as_row(resid, c0), as_row(c1, c2)], axis=0)

    def start_both(rights, lefts):
        @pl.when(not_last)
        def _():
            for copy in rights:
                copy.start()

        @pl.when(not_first)
        def _():
            for copy in lefts:
                copy.start()

    def wait_both(rights, lefts):
        @pl.when(not_first)
        def _():
            for copy in rights:
                copy.wait_recv()

        @pl.when(not_last)
        def _():
            for copy in lefts:
                copy.wait_recv()

    def half(k):
        return k // 2, slice((k % 2) * LANES, (k % 2 + 1) * LANES)

    @pl.when(me == 0)
    def _():
        for ref in (lowl_v, tl_v, psil_v, nzl_v):
            ref[...] = jnp.zeros_like(ref) if ref is not psil_v else jnp.ones_like(ref)

    @pl.when(me == nblk - 1)
    def _():
        for ref in (lowr_v, tr_v, psir_v, nzr_v):
            ref[...] = jnp.zeros_like(ref) if ref is not psir_v else jnp.ones_like(ref)

    zero = jnp.zeros((64, LANES), F32)
    loads[0].wait()
    acc = zero
    for k in range(NB):
        b = bh_v[:, cols(k)]
        acc = acc + b * b
    loads[1].wait()
    loads[2].wait()
    for k in range(NB):
        psi = psi_v[:, cols(k)]
        sh_v[:, cols(k)] = psi / (psi + TINY)
    rows = coefficients(0, lambda k: bh_v[:, cols(k)], acc)
    @pl.when(mc == 0)
    def _():
        pl.semaphore_wait(barrier, nblk - 1)
        pl.semaphore_signal(go_sem, inc=1, device_id={"blk": partner}, device_id_type=MESH)

    @pl.when(mc == 1)
    def _():
        pl.semaphore_wait(go_sem, 1)

    scale_start(0, rows)

    @pl.when(mc == 1)
    def _():
        for dz in range(1, nz):
            pl.semaphore_signal(barrier, inc=1, device_id={"phe": (mz + dz) % nz}, device_id_type=MESH)

    early = [
        remote(psi_v, psil_v, ws_sem.at[0], wr_sem.at[0], {"blk": right_peer}),
        remote(psi_v, psir_v, ws_sem.at[1], wr_sem.at[1], {"blk": left_peer}),
        remote(nz_v.at[1], nzl_v, ws_sem.at[2], wr_sem.at[2], {"blk": right_peer}),
        remote(nz_v.at[1], nzr_v, ws_sem.at[3], wr_sem.at[3], {"blk": left_peer}),
    ]
    start_both(early[2:3], early[3:4])

    for copy in loads[3:]:
        copy.wait()
    base = me * snps
    sub = lax.broadcasted_iota(jnp.int32, (LANES, snps), 0)
    for i in range(NB):
        rows = slice(i * LANES, (i + 1) * LANES)
        first = bf_s[i * LANES]
        last = bf_s[i * LANES + LANES - 1]
        tile = ld_v[rows, :].astype(F32)
        ra = pltpu.roll(tile, first & (snps - 1), axis=1)
        rb = pltpu.roll(tile, last & (snps - 1), axis=1)
        split = jnp.where(last == first, LANES, last - base - i * LANES)
        rt_m[:, rows] = jnp.where(sub >= split, rb, ra).T.astype(BF16)
    begin = bf_s[0]
    end = bf_s[snps - 1]
    from_left = jnp.where(begin < base, begin & (snps - 1), snps)
    to_right = jnp.where(not_last, end & (snps - 1), 0)
    lane = lax.broadcasted_iota(jnp.int32, (64, LANES), 1)

    ss = ss_v[...].astype(F32)
    ss2 = jnp.concatenate([ss, ss], axis=1)

    both = scale_sums(0)
    amp_row = amplitude(both[0:1])
    amp = as_col(amp_row)
    halo = []
    for k in range(NCH):
        kr, kl = NCH - 1 - k, k
        a = remote(low_v.at[kr], lowl_v.at[kr], ls_sem.at[kr], lr_sem.at[kr], {"blk": right_peer})
        b = remote(low_v.at[kl], lowr_v.at[kl], qs_sem.at[kl], qr_sem.at[kl], {"blk": left_peer})
        halo.append((kr, kl, a, b))
    for k, (kr, kl, a, b) in enumerate(halo):
        if k < NCH // 2:
            for j in (2 * kr, 2 * kr + 1, 2 * kl, 2 * kl + 1):
                v = sh_v[:, cols(j)] * (bh_v[:, cols(j)] + amp * nz_v[0, :, cols(j)].astype(F32))
                beta_v[:, cols(j)] = v
                c, w = half(j)
                low_v[c, :, w] = v.astype(BF16)
        start_both([a], [b])
    start_both(early[0:1], early[1:2])

    @pl.when(mc == 1)
    def _():
        pl.semaphore_wait(barrier, nz - 1)

    total = scale_finish(0, both, amp_row)
    for k in range(NB):
        v = beta_v[:, cols(k)]
        x_v[0:64, cols(k)] = v.astype(BF16)
        x_v[64:128, cols(k)] = jnp.where(lane + k * LANES < from_left, v, 0.0).astype(BF16)
        x_v[128:192, cols(k)] = jnp.where(lane + k * LANES >= to_right, v, 0.0).astype(BF16)
    acc_v[...] = jnp.dot(x_v[...], rt_m[...], preferred_element_type=F32)
    for kr, kl, a, b in halo:
        wait_both([a], [])
        q = lax.broadcasted_iota(jnp.int32, (64, CH), 1)
        x = jnp.where(q + kr * CH >= from_left, lowl_v[kr].astype(F32), 0.0).astype(BF16)
        upto = slice(0, (kr + 1) * CH)
        acc_v[64:128, upto] += jnp.dot(x, rt_m[kr * CH:(kr + 1) * CH, upto], preferred_element_type=F32)
        wait_both([], [b])
        x = jnp.where(q + kl * CH < to_right, lowr_v[kl].astype(F32), 0.0).astype(BF16)
        upto = slice(kl * CH, snps)
        acc_v[128:192, upto] += jnp.dot(x, rt_m[kl * CH:(kl + 1) * CH, upto], preferred_element_type=F32)

    def gradient(k):
        first = bf_v[:, cols(k)]
        applied = jnp.where(
            first < base, acc_v[64:128, cols(k)],
            jnp.where(first == end, acc_v[128:192, cols(k)], acc_v[0:64, cols(k)]),
        )
        return bh_v[:, cols(k)] - applied

    racc = zero
    for k in range(NB):
        g = gradient(k)
        racc = racc + g * g
        c, w = half(k)
        t_v[c, :, w] = beta_v[:, cols(k)] + g
    resid_start(0, as_row(racc, zero))

    sums = []
    for k in range(NCH):
        kr, kl = NCH - 1 - k, k
        sums.append(remote(t_v.at[kr], tl_v.at[kr], ts_sem.at[kr], tr_sem.at[kr], {"blk": right_peer}))
        sums.append(remote(t_v.at[kl], tr_v.at[kl], hs_sem.at[kl], hr_sem.at[kl], {"blk": left_peer}))

    late = mz >= nz // 2

    @pl.when(jnp.logical_not(late))
    def _():
        start_both(sums[0::2], sums[1::2])

    phi = phi_finish(0, total)
    for k in range(NB):
        psi = psi_v[:, cols(k)]
        sh_v[:, cols(k)] = psi / (psi + phi)

    def t_of(k):
        c, w = half(k)
        return t_v[c, :, w]

    scale_start(1, coefficients(1, t_of, zero))

    @pl.when(late)
    def _():
        start_both(sums[0::2], sums[1::2])

    wait_both(early[0::2], early[1::2])
    for k in range(NB):
        psi = psil_v[:, cols(k)]
        shl_v[:, cols(k)] = psi / (psi + phi)
        psi = psir_v[:, cols(k)]
        shr_v[:, cols(k)] = psi / (psi + phi)

    amp_row = resid_finish(0)
    amp = as_col(amp_row)

    @pl.when(late)
    def _():
        total_v[...] = scale_finish(1, scale_sums(1), amp_row)

    wait_both(sums[0::2], sums[1::2])
    for k in range(NB):
        c, w = half(k)
        b = sh_v[:, cols(k)] * (t_v[c, :, w] + amp * nz_v[1, :, cols(k)].astype(F32))
        bl = shl_v[:, cols(k)] * (tl_v[c, :, w] + amp * nzl_v[:, cols(k)].astype(F32))
        br = shr_v[:, cols(k)] * (tr_v[c, :, w] + amp * nzr_v[:, cols(k)].astype(F32))
        beta_v[:, cols(k)] = b
        x_v[0:64, cols(k)] = b.astype(BF16)
        x_v[64:128, cols(k)] = jnp.where(lane + k * LANES < from_left, b, bl).astype(BF16)
        x_v[128:192, cols(k)] = jnp.where(lane + k * LANES >= to_right, b, br).astype(BF16)
    acc_v[...] = jnp.dot(x_v[...], rt_m[...], preferred_element_type=F32)
    racc = zero
    for k in range(NB):
        g = gradient(k)
        racc = racc + g * g
        tail_v[:, cols(k)] = beta_v[:, cols(k)] + g
    resid_start(1, as_row(racc, zero))

    @pl.when(jnp.logical_not(late))
    def _():
        total_v[...] = scale_finish(1, scale_sums(1), amp_row)

    phi = phi_finish(1, total_v[...])
    for k in range(NB):
        psi = psi_v[:, cols(k)]
        shrink = psi / (psi + phi)
        u_v[:, cols(k)] = shrink * tail_v[:, cols(k)]
        v_v[:, cols(k)] = shrink * nz_v[2, :, cols(k)].astype(F32)

    for h in range(ITERS - 1):
        bytes_wait(rbuf.at[h, pl.ds(0, nblk - 1)], rs_sem.at[h])
        bytes_wait(sbuf.at[h, pl.ds(0, 2 * nblk - 2)], ss_sem.at[h])

    @pl.when(mc == 1)
    def _():
        for h in range(ITERS - 1):
            for _ in range(2):
                bytes_wait(pbuf.at[h, pl.ds(0, nz - 1)], ps_sem.at[h])

    @pl.when(not_last)
    def _():
        for copy in early[0::2] + sums[0::2] + [a for _, _, a, _ in halo]:
            copy.wait_send()

    @pl.when(not_first)
    def _():
        for copy in early[1::2] + sums[1::2] + [b for _, _, _, b in halo]:
            copy.wait_send()

    amp = as_col(resid_finish(1))
    for k in range(NB):
        out_ref[:, cols(k)] = u_v[:, cols(k)] + amp * v_v[:, cols(k)]


def shards(nx, ny, nz, ld_rows, block_first, beta_hat, psi, noise, sample_size):
    snps = ld_rows.shape[0]
    pheno = beta_hat.shape[0]
    V, dma = pltpu.VMEM, pltpu.SemaphoreType.DMA
    h = ITERS - 1
    nblk = nx * ny * 2
    wide = V((pheno, snps), F32)
    chunks = V((NCH, pheno, CH), F32)
    low = V((NCH, pheno, CH), BF16)
    thin = V((pheno, snps), BF16)
    four = dma((NCH,))
    arrays = (ld_rows, block_first, block_first.reshape(1, snps), beta_hat, psi, noise, sample_size.reshape(1, pheno))
    return pl.pallas_call(
        functools.partial(kernel, nx, ny, nz, snps),
        out_shape=pltpu.VMEM((pheno, snps), F32),
        in_specs=[pl.BlockSpec(memory_space=pl.ANY)] * 7,
        out_specs=pl.BlockSpec(memory_space=pltpu.VMEM),
        scratch_shapes=[
            V((snps, snps), BF16), pltpu.SMEM((snps,), jnp.int32), V((1, snps), jnp.int32), wide, wide,
            V((ITERS, pheno, snps), BF16), V((1, pheno), jnp.int32),
            V((snps, snps), BF16), V((3 * pheno, snps), BF16), V((3 * pheno, snps), F32), wide, wide, wide, wide, wide,
            low, low, low, chunks, chunks, chunks, wide, wide, thin, thin, wide, wide,
            V((h, nblk, LANES), F32), V((h, 2 * nblk, LANES), F32), V((h, nz, LANES), F32),
            V((1, LANES), F32),
            dma((7,)), dma((h,)), dma((h,)), dma((h,)), dma((h,)), dma((h,)), dma((h,)),
            four, four, four, four, four, four, four, four, four, four, pltpu.SemaphoreType.REGULAR,
        ],
        compiler_params=pltpu.CompilerParams(collective_id=0, has_side_effects=True, vmem_limit_bytes=32 * 1024 * 1024),
        name="shrinkage",
    )(*[pltpu.with_memory_space_constraint(a, pltpu.HBM) for a in arrays])


def solution(mesh):
    in_specs = (
        P("blk", None),
        P("blk"),
        P("phe", "blk"),
        P("phe", "blk"),
        P(None, "phe", "blk"),
        P("phe"),
    )
    body = functools.partial(shards, 4, mesh.shape["blk"] // 8, mesh.shape["phe"])
    return jax.shard_map(body, mesh=mesh, in_specs=in_specs, out_specs=P("phe", "blk"), check_vma=False)
```

```python
import functools

import jax
import jax.numpy as jnp
from jax import lax
from jax.experimental import pallas as pl
from jax.experimental.pallas import tpu as pltpu
from jax.sharding import PartitionSpec as P

ITERS = 3
TINY = 1e-06
SAMPLE_REF = 20000.0
MESH = pl.DeviceIdType.MESH
LANES = 128
NB = 8
CH = 256
NCH = 4
F32 = jnp.float32
BF16 = jnp.bfloat16


def peer_offsets(nx, ny):
    def hops(d):
        dx, dy, dc = d
        return min(dx, nx - dx) + min(dy, ny - dy) + 0.2 * dc

    every = [(dx, dy, dc) for dx in range(nx) for dy in range(ny) for dc in range(2)]
    return sorted([d for d in every if d != (0, 0, 0)], key=lambda d: -hops(d))


def kernel(
    nx, ny, nz, snps,
    ld_hbm, bf_hbm, bfr_hbm, bh_hbm, psi_hbm, nz_hbm, ss_hbm,
    out_ref,
    ld_v, bf_s, bf_v, bh_v, psi_v, nz_v, ss_v,
    rt_m, x_v, acc_v, tail_v, beta_v, sh_v, u_v, v_v,
    low_v, lowl_v, lowr_v, t_v, tl_v, tr_v, psil_v, psir_v, nzl_v, nzr_v, shl_v, shr_v,
    rbuf, sbuf, pbuf, scale_v, amp_v,
    in_sem, rs_sem, rr_sem, ss_sem, sr_sem, ps_sem, pr_sem,
    ls_sem, lr_sem, qs_sem, qr_sem, ts_sem, tr_sem, ws_sem, wr_sem, hs_sem, hr_sem, go_sem,
):
    nblk = nx * ny * 2
    me = lax.axis_index("blk")
    mz = lax.axis_index("phe")
    mx, my, mc = me // (2 * ny), (me // 2) % ny, me % 2
    offsets = peer_offsets(nx, ny)
    right_peer = (me + 1) % nblk
    left_peer = (me + nblk - 1) % nblk
    nsnp = float(snps * nblk)

    def blk_of(d):
        dx, dy, dc = d
        return ((mx + dx) % nx) * (2 * ny) + ((my + dy) % ny) * 2 + (mc + dc) % 2

    barrier = pltpu.get_barrier_semaphore()
    partner = me + 1 - 2 * mc
    late = mz >= nz // 2
    ahead = jnp.logical_not(late)
    not_first = me > 0
    not_last = me < nblk - 1
    for d in offsets:
        if d[2] == 0:
            chip = blk_of(d) // 2
            pl.semaphore_signal(barrier, inc=1, device_id={"blk": 2 * chip}, device_id_type=MESH)

    @pl.when(mc == 1)
    def _():
        pl.semaphore_signal(barrier, inc=1, device_id={"blk": partner}, device_id_type=MESH)

    loads = [
        pltpu.make_async_copy(bh_hbm, bh_v, in_sem.at[0]),
        pltpu.make_async_copy(psi_hbm, psi_v, in_sem.at[1]),
        pltpu.make_async_copy(nz_hbm, nz_v, in_sem.at[2]),
        pltpu.make_async_copy(bf_hbm, bf_s, in_sem.at[3]),
        pltpu.make_async_copy(bfr_hbm, bf_v, in_sem.at[4]),
        pltpu.make_async_copy(ss_hbm, ss_v, in_sem.at[5]),
        pltpu.make_async_copy(ld_hbm, ld_v, in_sem.at[6]),
    ]
    for copy in loads:
        copy.start()

    def cols(k):
        return slice(k * LANES, (k + 1) * LANES)

    def as_row(first, second):
        both = jnp.concatenate([first, second], axis=0)
        return jnp.sum(both.T, axis=0, keepdims=True)

    def as_col(row):
        return jnp.broadcast_to(row, (LANES, LANES)).T[:64]

    def remote(src, dst, ssem, rsem, who):
        return pltpu.make_async_remote_copy(src, dst, ssem, rsem, device_id=who, device_id_type=MESH)

    def bytes_wait(ref, sem):
        pltpu.make_async_copy(ref, ref, sem).wait()

    def to_all(ref, ssem, rsem):
        for d in offsets:
            remote(ref, ref, ssem, rsem, {"blk": blk_of(d)}).start()

    def resid_start(t, row):
        rbuf[t, pl.ds(me, 1)] = row
        to_all(rbuf.at[t, pl.ds(me, 1)], rs_sem.at[t], rr_sem.at[t])

    def resid_finish(t):
        bytes_wait(rbuf.at[t, pl.ds(0, nblk - 1)], rr_sem.at[t])
        return amplitude(jnp.sum(rbuf[t], axis=0, keepdims=True))

    def amplitude(total):
        return jnp.sqrt((total / nsnp + TINY) * SAMPLE_REF / ss2)

    def scale_start(h, rows):
        sbuf[h, pl.ds(2 * me, 2)] = rows
        to_all(sbuf.at[h, pl.ds(2 * me, 2)], ss_sem.at[h], sr_sem.at[h])

    def scale_sums(h):
        bytes_wait(sbuf.at[h, pl.ds(0, 2 * nblk - 2)], sr_sem.at[h])
        return jnp.sum(sbuf[h].reshape(nblk, 2, LANES), axis=0)

    def scale_finish(h, both, amp):
        c0 = pltpu.roll(both[0:1], 64, axis=1)
        c1 = both[1:2]
        c2 = pltpu.roll(both[1:2], 64, axis=1)
        lane = lax.broadcasted_iota(jnp.int32, (1, LANES), 1)
        total = jnp.where(lane < 64, jnp.maximum(c0 + 2.0 * amp * c1 + amp * amp * c2, 0.0), 0.0)
        mine = jnp.sum(total, axis=1, keepdims=True)
        pbuf[h, pl.ds(mz, 1)] = jnp.broadcast_to(mine, (1, LANES))

        @pl.when(mc == 1)
        def _():
            slot = pbuf.at[h, pl.ds(mz, 1)]
            for blk in (partner, me):
                for dz in sorted(range(1, nz), key=lambda d: -min(d, nz - d)):
                    who = {"blk": blk, "phe": (mz + dz) % nz}
                    remote(slot, slot, ps_sem.at[h], pr_sem.at[h], who).start()

        scale_v[...] = as_col(total / nsnp + TINY)

    def phi_finish(h):
        bytes_wait(pbuf.at[h, pl.ds(0, nz - 1)], pr_sem.at[h])
        pooled = jnp.sum(pbuf[h], axis=0, keepdims=True) / (nsnp * (64 * nz)) + TINY
        return (scale_v[...] + pooled) / 2.0

    def coefficients(t, value, resid):
        zero = jnp.zeros((64, LANES), F32)
        c0, c1, c2 = zero, zero, zero
        for k in range(NB):
            s = sh_v[:, cols(k)]
            w = s * s / psi_v[:, cols(k)]
            x = value(k)
            n = nz_v[t, :, cols(k)].astype(F32)
            c0 = c0 + w * x * x
            c1 = c1 + w * x * n
            c2 = c2 + w * n * n
        return jnp.concatenate([as_row(resid, c0), as_row(c1, c2)], axis=0)

    def start_both(rights, lefts):
        @pl.when(not_last)
        def _():
            for copy in rights:
                copy.start()

        @pl.when(not_first)
        def _():
            for copy in lefts:
                copy.start()

    def wait_both(rights, lefts):
        @pl.when(not_first)
        def _():
            for copy in rights:
                copy.wait_recv()

        @pl.when(not_last)
        def _():
            for copy in lefts:
                copy.wait_recv()

    def half(k):
        return k // 2, slice((k % 2) * LANES, (k % 2 + 1) * LANES)

    @pl.when(me == 0)
    def _():
        for ref in (lowl_v, tl_v, psil_v, nzl_v):
            ref[...] = jnp.zeros_like(ref) if ref is not psil_v else jnp.ones_like(ref)

    @pl.when(me == nblk - 1)
    def _():
        for ref in (lowr_v, tr_v, psir_v, nzr_v):
            ref[...] = jnp.zeros_like(ref) if ref is not psir_v else jnp.ones_like(ref)

    zero = jnp.zeros((64, LANES), F32)
    loads[0].wait()
    acc = zero
    for k in range(NB):
        b = bh_v[:, cols(k)]
        acc = acc + b * b
    loads[1].wait()
    loads[2].wait()
    for k in range(NB):
        psi = psi_v[:, cols(k)]
        sh_v[:, cols(k)] = psi / (psi + TINY)
    rows = coefficients(0, lambda k: bh_v[:, cols(k)], acc)
    @pl.when(mc == 0)
    def _():
        pl.semaphore_wait(barrier, nblk - 1)
        pl.semaphore_signal(go_sem, inc=1, device_id={"blk": partner}, device_id_type=MESH)

    @pl.when(mc == 1)
    def _():
        pl.semaphore_wait(go_sem, 1)

    scale_start(0, rows)

    @pl.when(mc == 1)
    def _():
        for dz in range(1, nz):
            pl.semaphore_signal(barrier, inc=1, device_id={"phe": (mz + dz) % nz}, device_id_type=MESH)

    early = [
        remote(psi_v, psil_v, ws_sem.at[0], wr_sem.at[0], {"blk": right_peer}),
        remote(psi_v, psir_v, ws_sem.at[1], wr_sem.at[1], {"blk": left_peer}),
        remote(nz_v.at[1], nzl_v, ws_sem.at[2], wr_sem.at[2], {"blk": right_peer}),
        remote(nz_v.at[1], nzr_v, ws_sem.at[3], wr_sem.at[3], {"blk": left_peer}),
    ]
    start_both(early[2:3], early[3:4])

    for copy in loads[3:]:
        copy.wait()
    base = me * snps
    sub = lax.broadcasted_iota(jnp.int32, (LANES, snps), 0)
    for i in range(NB):
        rows = slice(i * LANES, (i + 1) * LANES)
        first = bf_s[i * LANES]
        last = bf_s[i * LANES + LANES - 1]
        tile = ld_v[rows, :].astype(F32)
        ra = pltpu.roll(tile, first & (snps - 1), axis=1)
        rb = pltpu.roll(tile, last & (snps - 1), axis=1)
        split = jnp.where(last == first, LANES, last - base - i * LANES)
        rt_m[:, rows] = jnp.where(sub >= split, rb, ra).T.astype(BF16)
    begin = bf_s[0]
    end = bf_s[snps - 1]
    from_left = jnp.where(begin < base, begin & (snps - 1), snps)
    to_right = jnp.where(not_last, end & (snps - 1), 0)
    lane = lax.broadcasted_iota(jnp.int32, (64, LANES), 1)

    ss = ss_v[...].astype(F32)
    ss2 = jnp.concatenate([ss, ss], axis=1)

    both = scale_sums(0)
    amp_row = amplitude(both[0:1])
    amp = as_col(amp_row)
    halo = []
    for k in range(NCH):
        kr, kl = NCH - 1 - k, k
        a = remote(low_v.at[kr], lowl_v.at[kr], ls_sem.at[kr], lr_sem.at[kr], {"blk": right_peer})
        b = remote(low_v.at[kl], lowr_v.at[kl], qs_sem.at[kl], qr_sem.at[kl], {"blk": left_peer})
        halo.append((kr, kl, a, b))
    def pool():
        @pl.when(mc == 1)
        def _():
            pl.semaphore_wait(barrier, nz - 1)

        scale_finish(0, both, amp_row)

    for k, (kr, kl, a, b) in enumerate(halo):
        if k < NCH // 2:
            for j in (2 * kr, 2 * kr + 1, 2 * kl, 2 * kl + 1):
                v = sh_v[:, cols(j)] * (bh_v[:, cols(j)] + amp * nz_v[0, :, cols(j)].astype(F32))
                beta_v[:, cols(j)] = v
                c, w = half(j)
                low_v[c, :, w] = v.astype(BF16)
        start_both([a], [b])
        if k == 0:
            pl.when(late)(pool)
    start_both(early[0:1], early[1:2])
    pl.when(ahead)(pool)

    for k in range(NB):
        v = beta_v[:, cols(k)]
        x_v[0:64, cols(k)] = v.astype(BF16)
        x_v[64:128, cols(k)] = jnp.where(lane + k * LANES < from_left, v, 0.0).astype(BF16)
        x_v[128:192, cols(k)] = jnp.where(lane + k * LANES >= to_right, v, 0.0).astype(BF16)
    acc_v[...] = jnp.dot(x_v[...], rt_m[...], preferred_element_type=F32)
    for kr, kl, a, b in halo:
        wait_both([a], [])
        q = lax.broadcasted_iota(jnp.int32, (64, CH), 1)
        x = jnp.where(q + kr * CH >= from_left, lowl_v[kr].astype(F32), 0.0).astype(BF16)
        upto = slice(0, (kr + 1) * CH)
        acc_v[64:128, upto] += jnp.dot(x, rt_m[kr * CH:(kr + 1) * CH, upto], preferred_element_type=F32)
        wait_both([], [b])
        x = jnp.where(q + kl * CH < to_right, lowr_v[kl].astype(F32), 0.0).astype(BF16)
        upto = slice(kl * CH, snps)
        acc_v[128:192, upto] += jnp.dot(x, rt_m[kl * CH:(kl + 1) * CH, upto], preferred_element_type=F32)

    def gradient(k):
        first = bf_v[:, cols(k)]
        applied = jnp.where(
            first < base, acc_v[64:128, cols(k)],
            jnp.where(first == end, acc_v[128:192, cols(k)], acc_v[0:64, cols(k)]),
        )
        return bh_v[:, cols(k)] - applied

    racc = zero
    for k in range(NB):
        g = gradient(k)
        racc = racc + g * g
        c, w = half(k)
        t_v[c, :, w] = beta_v[:, cols(k)] + g

    sums = []
    for k in range(NCH):
        kr, kl = NCH - 1 - k, k
        sums.append(remote(t_v.at[kr], tl_v.at[kr], ts_sem.at[kr], tr_sem.at[kr], {"blk": right_peer}))
        sums.append(remote(t_v.at[kl], tr_v.at[kl], hs_sem.at[kl], hr_sem.at[kl], {"blk": left_peer}))

    @pl.when(ahead)
    def _():
        resid_start(0, as_row(racc, zero))
        start_both(sums[0::2], sums[1::2])

    phi = phi_finish(0)
    for k in range(NB):
        psi = psi_v[:, cols(k)]
        sh_v[:, cols(k)] = psi / (psi + phi)

    def t_of(k):
        c, w = half(k)
        return t_v[c, :, w]

    scale_start(1, coefficients(1, t_of, racc))

    @pl.when(late)
    def _():
        start_both(sums[0::2], sums[1::2])

    wait_both(early[0::2], early[1::2])
    for k in range(NB):
        psi = psil_v[:, cols(k)]
        shl_v[:, cols(k)] = psi / (psi + phi)
        psi = psir_v[:, cols(k)]
        shr_v[:, cols(k)] = psi / (psi + phi)

    @pl.when(ahead)
    def _():
        amp_v[...] = resid_finish(0)

    @pl.when(late)
    def _():
        both = scale_sums(1)
        amp_v[...] = amplitude(both[0:1])
        scale_finish(1, both, amp_v[...])

    amp_row = amp_v[...]
    amp = as_col(amp_row)
    wait_both(sums[0::2], sums[1::2])
    for k in range(NB):
        c, w = half(k)
        b = sh_v[:, cols(k)] * (t_v[c, :, w] + amp * nz_v[1, :, cols(k)].astype(F32))
        bl = shl_v[:, cols(k)] * (tl_v[c, :, w] + amp * nzl_v[:, cols(k)].astype(F32))
        br = shr_v[:, cols(k)] * (tr_v[c, :, w] + amp * nzr_v[:, cols(k)].astype(F32))
        beta_v[:, cols(k)] = b
        x_v[0:64, cols(k)] = b.astype(BF16)
        x_v[64:128, cols(k)] = jnp.where(lane + k * LANES < from_left, b, bl).astype(BF16)
        x_v[128:192, cols(k)] = jnp.where(lane + k * LANES >= to_right, b, br).astype(BF16)
    acc_v[...] = jnp.dot(x_v[...], rt_m[...], preferred_element_type=F32)
    racc = zero
    for k in range(NB):
        g = gradient(k)
        racc = racc + g * g
        tail_v[:, cols(k)] = beta_v[:, cols(k)] + g
    resid_start(1, as_row(racc, zero))

    def drain():
        @pl.when(ahead)
        def _():
            bytes_wait(rbuf.at[0, pl.ds(0, nblk - 1)], rs_sem.at[0])

        bytes_wait(rbuf.at[1, pl.ds(0, nblk - 1)], rs_sem.at[1])
        for h in range(ITERS - 1):
            bytes_wait(sbuf.at[h, pl.ds(0, 2 * nblk - 2)], ss_sem.at[h])

        @pl.when(mc == 1)
        def _():
            for h in range(ITERS - 1):
                for _ in range(2):
                    bytes_wait(pbuf.at[h, pl.ds(0, nz - 1)], ps_sem.at[h])

        @pl.when(not_last)
        def _():
            for copy in early[0::2] + sums[0::2] + [a for _, _, a, _ in halo]:
                copy.wait_send()

        @pl.when(not_first)
        def _():
            for copy in early[1::2] + sums[1::2] + [b for _, _, _, b in halo]:
                copy.wait_send()

    def noise_of(k):
        return nz_v[ITERS - 1, :, cols(k)].astype(F32)

    @pl.when(ahead)
    def _():
        scale_finish(1, scale_sums(1), amp_row)
        amp = as_col(resid_finish(1))
        for k in range(NB):
            u_v[:, cols(k)] = tail_v[:, cols(k)] + amp * noise_of(k)
        drain()
        phi = phi_finish(1)
        for k in range(NB):
            psi = psi_v[:, cols(k)]
            out_ref[:, cols(k)] = psi / (psi + phi) * u_v[:, cols(k)]

    @pl.when(late)
    def _():
        phi = phi_finish(1)
        for k in range(NB):
            psi = psi_v[:, cols(k)]
            shrink = psi / (psi + phi)
            u_v[:, cols(k)] = shrink * tail_v[:, cols(k)]
            v_v[:, cols(k)] = shrink * noise_of(k)
        drain()
        amp = as_col(resid_finish(1))
        for k in range(NB):
            out_ref[:, cols(k)] = u_v[:, cols(k)] + amp * v_v[:, cols(k)]


def shards(nx, ny, nz, ld_rows, block_first, beta_hat, psi, noise, sample_size):
    snps = ld_rows.shape[0]
    pheno = beta_hat.shape[0]
    V, dma = pltpu.VMEM, pltpu.SemaphoreType.DMA
    h = ITERS - 1
    nblk = nx * ny * 2
    wide = V((pheno, snps), F32)
    chunks = V((NCH, pheno, CH), F32)
    low = V((NCH, pheno, CH), BF16)
    thin = V((pheno, snps), BF16)
    four = dma((NCH,))
    arrays = (ld_rows, block_first, block_first.reshape(1, snps), beta_hat, psi, noise, sample_size.reshape(1, pheno))
    return pl.pallas_call(
        functools.partial(kernel, nx, ny, nz, snps),
        out_shape=pltpu.VMEM((pheno, snps), F32),
        in_specs=[pl.BlockSpec(memory_space=pl.ANY)] * 7,
        out_specs=pl.BlockSpec(memory_space=pltpu.VMEM),
        scratch_shapes=[
            V((snps, snps), BF16), pltpu.SMEM((snps,), jnp.int32), V((1, snps), jnp.int32), wide, wide,
            V((ITERS, pheno, snps), BF16), V((1, pheno), jnp.int32),
            V((snps, snps), BF16), V((3 * pheno, snps), BF16), V((3 * pheno, snps), F32), wide, wide, wide, wide, wide,
            low, low, low, chunks, chunks, chunks, wide, wide, thin, thin, wide, wide,
            V((h, nblk, LANES), F32), V((h, 2 * nblk, LANES), F32), V((h, nz, LANES), F32),
            V((pheno, LANES), F32), V((1, LANES), F32),
            dma((7,)), dma((h,)), dma((h,)), dma((h,)), dma((h,)), dma((h,)), dma((h,)),
            four, four, four, four, four, four, four, four, four, four, pltpu.SemaphoreType.REGULAR,
        ],
        compiler_params=pltpu.CompilerParams(collective_id=0, has_side_effects=True, vmem_limit_bytes=32 * 1024 * 1024),
        name="shrinkage",
    )(*[pltpu.with_memory_space_constraint(a, pltpu.HBM) for a in arrays])


def solution(mesh):
    in_specs = (
        P("blk", None),
        P("blk"),
        P("phe", "blk"),
        P("phe", "blk"),
        P(None, "phe", "blk"),
        P("phe"),
    )
    body = functools.partial(shards, 4, mesh.shape["blk"] // 8, mesh.shape["phe"])
    return jax.shard_map(body, mesh=mesh, in_specs=in_specs, out_specs=P("phe", "blk"), check_vma=False)
```

```python
import functools

import jax
import jax.numpy as jnp
from jax import lax
from jax.experimental import pallas as pl
from jax.experimental.pallas import tpu as pltpu
from jax.sharding import PartitionSpec as P

ITERS = 3
TINY = 1e-06
SAMPLE_REF = 20000.0
MESH = pl.DeviceIdType.MESH
LANES = 128
NB = 8
CH = 256
NCH = 4
F32 = jnp.float32
BF16 = jnp.bfloat16


def peer_offsets(nx, ny):
    def hops(d):
        dx, dy, dc = d
        return min(dx, nx - dx) + min(dy, ny - dy) + 0.2 * dc

    every = [(dx, dy, dc) for dx in range(nx) for dy in range(ny) for dc in range(2)]
    return sorted([d for d in every if d != (0, 0, 0)], key=lambda d: -hops(d))


def kernel(
    nx, ny, nz, snps,
    ld_hbm, bf_hbm, bfr_hbm, bh_hbm, psi_hbm, nz_hbm, ss_hbm,
    out_ref,
    ld_v, bf_s, bf_v, bh_v, psi_v, nz_v, ss_v,
    rt_m, x_v, acc_v, tail_v, beta_v, sh_v, u_v, v_v,
    low_v, lowl_v, lowr_v, t_v, tl_v, tr_v, psil_v, psir_v, nzl_v, nzr_v, shl_v, shr_v,
    rbuf, sbuf, pbuf, scale_v, amp_v,
    in_sem, rs_sem, rr_sem, ss_sem, sr_sem, ps_sem, pr_sem,
    ls_sem, lr_sem, qs_sem, qr_sem, ts_sem, tr_sem, ws_sem, wr_sem, hs_sem, hr_sem, go_sem,
):
    nblk = nx * ny * 2
    me = lax.axis_index("blk")
    mz = lax.axis_index("phe")
    mx, my, mc = me // (2 * ny), (me // 2) % ny, me % 2
    offsets = peer_offsets(nx, ny)
    right_peer = (me + 1) % nblk
    left_peer = (me + nblk - 1) % nblk
    nsnp = float(snps * nblk)

    def blk_of(d):
        dx, dy, dc = d
        return ((mx + dx) % nx) * (2 * ny) + ((my + dy) % ny) * 2 + (mc + dc) % 2

    barrier = pltpu.get_barrier_semaphore()
    partner = me + 1 - 2 * mc
    late = mz >= nz // 2
    ahead = jnp.logical_not(late)
    not_first = me > 0
    not_last = me < nblk - 1
    for d in offsets:
        if d[2] == 0:
            chip = blk_of(d) // 2
            pl.semaphore_signal(barrier, inc=1, device_id={"blk": 2 * chip}, device_id_type=MESH)

    @pl.when(mc == 1)
    def _():
        pl.semaphore_signal(barrier, inc=1, device_id={"blk": partner}, device_id_type=MESH)

    loads = [
        pltpu.make_async_copy(bh_hbm, bh_v, in_sem.at[0]),
        pltpu.make_async_copy(psi_hbm, psi_v, in_sem.at[1]),
        pltpu.make_async_copy(nz_hbm, nz_v, in_sem.at[2]),
        pltpu.make_async_copy(bf_hbm, bf_s, in_sem.at[3]),
        pltpu.make_async_copy(bfr_hbm, bf_v, in_sem.at[4]),
        pltpu.make_async_copy(ss_hbm, ss_v, in_sem.at[5]),
        pltpu.make_async_copy(ld_hbm, ld_v, in_sem.at[6]),
    ]
    for copy in loads:
        copy.start()

    def cols(k):
        return slice(k * LANES, (k + 1) * LANES)

    def as_row(first, second):
        both = jnp.concatenate([first, second], axis=0)
        return jnp.sum(both.T, axis=0, keepdims=True)

    def as_col(row):
        return jnp.broadcast_to(row, (LANES, LANES)).T[:64]

    def remote(src, dst, ssem, rsem, who):
        return pltpu.make_async_remote_copy(src, dst, ssem, rsem, device_id=who, device_id_type=MESH)

    def bytes_wait(ref, sem):
        pltpu.make_async_copy(ref, ref, sem).wait()

    def to_all(ref, ssem, rsem):
        for d in offsets:
            remote(ref, ref, ssem, rsem, {"blk": blk_of(d)}).start()

    def resid_start(t, row):
        rbuf[t, pl.ds(me, 1)] = row
        to_all(rbuf.at[t, pl.ds(me, 1)], rs_sem.at[t], rr_sem.at[t])

    def resid_finish(t):
        bytes_wait(rbuf.at[t, pl.ds(0, nblk - 1)], rr_sem.at[t])
        return amplitude(jnp.sum(rbuf[t], axis=0, keepdims=True))

    def amplitude(total):
        return jnp.sqrt((total / nsnp + TINY) * SAMPLE_REF / ss2)

    def scale_start(h, rows):
        sbuf[h, pl.ds(2 * me, 2)] = rows
        to_all(sbuf.at[h, pl.ds(2 * me, 2)], ss_sem.at[h], sr_sem.at[h])

    def scale_sums(h):
        bytes_wait(sbuf.at[h, pl.ds(0, 2 * nblk - 2)], sr_sem.at[h])
        return jnp.sum(sbuf[h].reshape(nblk, 2, LANES), axis=0)

    def scale_finish(h, both, amp):
        c0 = pltpu.roll(both[0:1], 64, axis=1)
        c1 = both[1:2]
        c2 = pltpu.roll(both[1:2], 64, axis=1)
        lane = lax.broadcasted_iota(jnp.int32, (1, LANES), 1)
        total = jnp.where(lane < 64, jnp.maximum(c0 + 2.0 * amp * c1 + amp * amp * c2, 0.0), 0.0)
        mine = jnp.sum(total, axis=1, keepdims=True)
        pbuf[h, pl.ds(mz, 1)] = jnp.broadcast_to(mine, (1, LANES))

        @pl.when(mc == 1)
        def _():
            slot = pbuf.at[h, pl.ds(mz, 1)]
            for dz in sorted(range(1, nz), key=lambda d: -min(d, nz - d)):
                for blk in (partner, me):
                    who = {"blk": blk, "phe": (mz + dz) % nz}
                    remote(slot, slot, ps_sem.at[h], pr_sem.at[h], who).start()

        scale_v[...] = as_col(total / nsnp + TINY)

    def phi_finish(h):
        bytes_wait(pbuf.at[h, pl.ds(0, nz - 1)], pr_sem.at[h])
        pooled = jnp.sum(pbuf[h], axis=0, keepdims=True) / (nsnp * (64 * nz)) + TINY
        return (scale_v[...] + pooled) / 2.0

    def coefficients(t, value, resid):
        zero = jnp.zeros((64, LANES), F32)
        c0, c1, c2 = zero, zero, zero
        for k in range(NB):
            s = sh_v[:, cols(k)]
            w = s * s / psi_v[:, cols(k)]
            x = value(k)
            n = nz_v[t, :, cols(k)].astype(F32)
            c0 = c0 + w * x * x
            c1 = c1 + w * x * n
            c2 = c2 + w * n * n
        return jnp.concatenate([as_row(resid, c0), as_row(c1, c2)], axis=0)

    def start_both(rights, lefts):
        @pl.when(not_last)
        def _():
            for copy in rights:
                copy.start()

        @pl.when(not_first)
        def _():
            for copy in lefts:
                copy.start()

    def wait_both(rights, lefts):
        @pl.when(not_first)
        def _():
            for copy in rights:
                copy.wait_recv()

        @pl.when(not_last)
        def _():
            for copy in lefts:
                copy.wait_recv()

    def half(k):
        return k // 2, slice((k % 2) * LANES, (k % 2 + 1) * LANES)

    @pl.when(me == 0)
    def _():
        for ref in (lowl_v, tl_v, psil_v, nzl_v):
            ref[...] = jnp.zeros_like(ref) if ref is not psil_v else jnp.ones_like(ref)

    @pl.when(me == nblk - 1)
    def _():
        for ref in (lowr_v, tr_v, psir_v, nzr_v):
            ref[...] = jnp.zeros_like(ref) if ref is not psir_v else jnp.ones_like(ref)

    zero = jnp.zeros((64, LANES), F32)
    loads[0].wait()
    acc = zero
    for k in range(NB):
        b = bh_v[:, cols(k)]
        acc = acc + b * b
    loads[1].wait()
    loads[2].wait()
    for k in range(NB):
        psi = psi_v[:, cols(k)]
        sh_v[:, cols(k)] = psi / (psi + TINY)
    rows = coefficients(0, lambda k: bh_v[:, cols(k)], acc)
    sbuf[0, pl.ds(2 * me, 2)] = rows

    @pl.when(mc == 0)
    def _():
        pl.semaphore_wait(barrier, nblk - 1)
        pl.semaphore_signal(go_sem, inc=1, device_id={"blk": partner}, device_id_type=MESH)

    @pl.when(mc == 1)
    def _():
        pl.semaphore_wait(go_sem, 1)

    to_all(sbuf.at[0, pl.ds(2 * me, 2)], ss_sem.at[0], sr_sem.at[0])

    @pl.when(mc == 1)
    def _():
        for dz in range(1, nz):
            pl.semaphore_signal(barrier, inc=1, device_id={"phe": (mz + dz) % nz}, device_id_type=MESH)

    early = [
        remote(psi_v, psil_v, ws_sem.at[0], wr_sem.at[0], {"blk": right_peer}),
        remote(psi_v, psir_v, ws_sem.at[1], wr_sem.at[1], {"blk": left_peer}),
        remote(nz_v.at[1], nzl_v, ws_sem.at[2], wr_sem.at[2], {"blk": right_peer}),
        remote(nz_v.at[1], nzr_v, ws_sem.at[3], wr_sem.at[3], {"blk": left_peer}),
    ]
    start_both(early[2:3], early[3:4])

    for copy in loads[3:]:
        copy.wait()
    base = me * snps
    sub = lax.broadcasted_iota(jnp.int32, (LANES, snps), 0)
    for i in range(NB):
        rows = slice(i * LANES, (i + 1) * LANES)
        first = bf_s[i * LANES]
        last = bf_s[i * LANES + LANES - 1]
        tile = ld_v[rows, :].astype(F32)
        ra = pltpu.roll(tile, first & (snps - 1), axis=1)
        rb = pltpu.roll(tile, last & (snps - 1), axis=1)
        split = jnp.where(last == first, LANES, last - base - i * LANES)
        rt_m[:, rows] = jnp.where(sub >= split, rb, ra).T.astype(BF16)
    begin = bf_s[0]
    end = bf_s[snps - 1]
    from_left = jnp.where(begin < base, begin & (snps - 1), snps)
    to_right = jnp.where(not_last, end & (snps - 1), 0)
    lane = lax.broadcasted_iota(jnp.int32, (64, LANES), 1)

    ss = ss_v[...].astype(F32)
    ss2 = jnp.concatenate([ss, ss], axis=1)

    both = scale_sums(0)
    amp_row = amplitude(both[0:1])
    amp = as_col(amp_row)
    halo = []
    for k in range(NCH):
        kr, kl = NCH - 1 - k, k
        a = remote(low_v.at[kr], lowl_v.at[kr], ls_sem.at[kr], lr_sem.at[kr], {"blk": right_peer})
        b = remote(low_v.at[kl], lowr_v.at[kl], qs_sem.at[kl], qr_sem.at[kl], {"blk": left_peer})
        halo.append((kr, kl, a, b))
    def pool():
        @pl.when(mc == 1)
        def _():
            pl.semaphore_wait(barrier, nz - 1)

        scale_finish(0, both, amp_row)

    for k, (kr, kl, a, b) in enumerate(halo):
        if k < NCH // 2:
            for j in (2 * kr, 2 * kr + 1, 2 * kl, 2 * kl + 1):
                v = sh_v[:, cols(j)] * (bh_v[:, cols(j)] + amp * nz_v[0, :, cols(j)].astype(F32))
                beta_v[:, cols(j)] = v
                c, w = half(j)
                low_v[c, :, w] = v.astype(BF16)
        start_both([a], [b])
        if k == 0:
            pl.when(late)(pool)
    start_both(early[0:1], early[1:2])
    pl.when(ahead)(pool)

    for k in range(NB):
        v = beta_v[:, cols(k)]
        x_v[0:64, cols(k)] = v.astype(BF16)
        x_v[64:128, cols(k)] = jnp.where(lane + k * LANES < from_left, v, 0.0).astype(BF16)
        x_v[128:192, cols(k)] = jnp.where(lane + k * LANES >= to_right, v, 0.0).astype(BF16)
    acc_v[...] = jnp.dot(x_v[...], rt_m[...], preferred_element_type=F32)
    for kr, kl, a, b in halo:
        wait_both([a], [])
        q = lax.broadcasted_iota(jnp.int32, (64, CH), 1)
        x = jnp.where(q + kr * CH >= from_left, lowl_v[kr].astype(F32), 0.0).astype(BF16)
        upto = slice(0, (kr + 1) * CH)
        acc_v[64:128, upto] += jnp.dot(x, rt_m[kr * CH:(kr + 1) * CH, upto], preferred_element_type=F32)
        wait_both([], [b])
        x = jnp.where(q + kl * CH < to_right, lowr_v[kl].astype(F32), 0.0).astype(BF16)
        upto = slice(kl * CH, snps)
        acc_v[128:192, upto] += jnp.dot(x, rt_m[kl * CH:(kl + 1) * CH, upto], preferred_element_type=F32)

    def gradient(k):
        first = bf_v[:, cols(k)]
        applied = jnp.where(
            first < base, acc_v[64:128, cols(k)],
            jnp.where(first == end, acc_v[128:192, cols(k)], acc_v[0:64, cols(k)]),
        )
        return bh_v[:, cols(k)] - applied

    racc = zero
    for k in range(NB):
        g = gradient(k)
        racc = racc + g * g
        c, w = half(k)
        t_v[c, :, w] = beta_v[:, cols(k)] + g

    sums = []
    for k in range(NCH):
        kr, kl = NCH - 1 - k, k
        sums.append(remote(t_v.at[kr], tl_v.at[kr], ts_sem.at[kr], tr_sem.at[kr], {"blk": right_peer}))
        sums.append(remote(t_v.at[kl], tr_v.at[kl], hs_sem.at[kl], hr_sem.at[kl], {"blk": left_peer}))

    @pl.when(ahead)
    def _():
        resid_start(0, as_row(racc, zero))
        start_both(sums[0::2], sums[1::2])

    phi = phi_finish(0)
    for k in range(NB):
        psi = psi_v[:, cols(k)]
        sh_v[:, cols(k)] = psi / (psi + phi)

    def t_of(k):
        c, w = half(k)
        return t_v[c, :, w]

    scale_start(1, coefficients(1, t_of, racc))

    @pl.when(late)
    def _():
        start_both(sums[0::2], sums[1::2])

    wait_both(early[0::2], early[1::2])
    for k in range(NB):
        psi = psil_v[:, cols(k)]
        shl_v[:, cols(k)] = psi / (psi + phi)
        psi = psir_v[:, cols(k)]
        shr_v[:, cols(k)] = psi / (psi + phi)

    @pl.when(ahead)
    def _():
        amp_v[...] = resid_finish(0)

    @pl.when(late)
    def _():
        both = scale_sums(1)
        amp_v[...] = amplitude(both[0:1])
        scale_finish(1, both, amp_v[...])

    amp_row = amp_v[...]
    amp = as_col(amp_row)
    wait_both(sums[0::2], sums[1::2])
    for k in range(NB):
        c, w = half(k)
        b = sh_v[:, cols(k)] * (t_v[c, :, w] + amp * nz_v[1, :, cols(k)].astype(F32))
        bl = shl_v[:, cols(k)] * (tl_v[c, :, w] + amp * nzl_v[:, cols(k)].astype(F32))
        br = shr_v[:, cols(k)] * (tr_v[c, :, w] + amp * nzr_v[:, cols(k)].astype(F32))
        beta_v[:, cols(k)] = b
        x_v[0:64, cols(k)] = b.astype(BF16)
        x_v[64:128, cols(k)] = jnp.where(lane + k * LANES < from_left, b, bl).astype(BF16)
        x_v[128:192, cols(k)] = jnp.where(lane + k * LANES >= to_right, b, br).astype(BF16)
    acc_v[...] = jnp.dot(x_v[...], rt_m[...], preferred_element_type=F32)
    racc = zero
    for k in range(NB):
        g = gradient(k)
        racc = racc + g * g
        tail_v[:, cols(k)] = beta_v[:, cols(k)] + g
    resid_start(1, as_row(racc, zero))

    def drain():
        @pl.when(ahead)
        def _():
            bytes_wait(rbuf.at[0, pl.ds(0, nblk - 1)], rs_sem.at[0])

        bytes_wait(rbuf.at[1, pl.ds(0, nblk - 1)], rs_sem.at[1])
        for h in range(ITERS - 1):
            bytes_wait(sbuf.at[h, pl.ds(0, 2 * nblk - 2)], ss_sem.at[h])

        @pl.when(mc == 1)
        def _():
            for h in range(ITERS - 1):
                for _ in range(2):
                    bytes_wait(pbuf.at[h, pl.ds(0, nz - 1)], ps_sem.at[h])

        @pl.when(not_last)
        def _():
            for copy in early[0::2] + sums[0::2] + [a for _, _, a, _ in halo]:
                copy.wait_send()

        @pl.when(not_first)
        def _():
            for copy in early[1::2] + sums[1::2] + [b for _, _, _, b in halo]:
                copy.wait_send()

    def noise_of(k):
        return nz_v[ITERS - 1, :, cols(k)].astype(F32)

    @pl.when(ahead)
    def _():
        scale_finish(1, scale_sums(1), amp_row)
        amp = as_col(resid_finish(1))
        for k in range(NB):
            u_v[:, cols(k)] = tail_v[:, cols(k)] + amp * noise_of(k)
        drain()
        phi = phi_finish(1)
        for k in range(NB):
            psi = psi_v[:, cols(k)]
            out_ref[:, cols(k)] = psi / (psi + phi) * u_v[:, cols(k)]

    @pl.when(late)
    def _():
        phi = phi_finish(1)
        for k in range(NB):
            psi = psi_v[:, cols(k)]
            shrink = psi / (psi + phi)
            u_v[:, cols(k)] = shrink * tail_v[:, cols(k)]
            v_v[:, cols(k)] = shrink * noise_of(k)
        drain()
        amp = as_col(resid_finish(1))
        for k in range(NB):
            out_ref[:, cols(k)] = u_v[:, cols(k)] + amp * v_v[:, cols(k)]


def shards(nx, ny, nz, ld_rows, block_first, beta_hat, psi, noise, sample_size):
    snps = ld_rows.shape[0]
    pheno = beta_hat.shape[0]
    V, dma = pltpu.VMEM, pltpu.SemaphoreType.DMA
    h = ITERS - 1
    nblk = nx * ny * 2
    wide = V((pheno, snps), F32)
    chunks = V((NCH, pheno, CH), F32)
    low = V((NCH, pheno, CH), BF16)
    thin = V((pheno, snps), BF16)
    four = dma((NCH,))
    arrays = (ld_rows, block_first, block_first.reshape(1, snps), beta_hat, psi, noise, sample_size.reshape(1, pheno))
    return pl.pallas_call(
        functools.partial(kernel, nx, ny, nz, snps),
        out_shape=pltpu.VMEM((pheno, snps), F32),
        in_specs=[pl.BlockSpec(memory_space=pl.ANY)] * 7,
        out_specs=pl.BlockSpec(memory_space=pltpu.VMEM),
        scratch_shapes=[
            V((snps, snps), BF16), pltpu.SMEM((snps,), jnp.int32), V((1, snps), jnp.int32), wide, wide,
            V((ITERS, pheno, snps), BF16), V((1, pheno), jnp.int32),
            V((snps, snps), BF16), V((3 * pheno, snps), BF16), V((3 * pheno, snps), F32), wide, wide, wide, wide, wide,
            low, low, low, chunks, chunks, chunks, wide, wide, thin, thin, wide, wide,
            V((h, nblk, LANES), F32), V((h, 2 * nblk, LANES), F32), V((h, nz, LANES), F32),
            V((pheno, LANES), F32), V((1, LANES), F32),
            dma((7,)), dma((h,)), dma((h,)), dma((h,)), dma((h,)), dma((h,)), dma((h,)),
            four, four, four, four, four, four, four, four, four, four, pltpu.SemaphoreType.REGULAR,
        ],
        compiler_params=pltpu.CompilerParams(collective_id=0, has_side_effects=True, vmem_limit_bytes=32 * 1024 * 1024),
        name="shrinkage",
    )(*[pltpu.with_memory_space_constraint(a, pltpu.HBM) for a in arrays])


def solution(mesh):
    in_specs = (
        P("blk", None),
        P("blk"),
        P("phe", "blk"),
        P("phe", "blk"),
        P(None, "phe", "blk"),
        P("phe"),
    )
    body = functools.partial(shards, 4, mesh.shape["blk"] // 8, mesh.shape["phe"])
    return jax.shard_map(body, mesh=mesh, in_specs=in_specs, out_specs=P("phe", "blk"), check_vma=False)
```
